32 devices in a mesh: rep: 1 (over z), model: 32 (over y, x, core).
Axes of the slice: x: 4, y: 4, z: 1, core: 2. Of those that a mesh axis runs over, the one named last changes fastest.
The devices are a block of a 4x4x8 slice.
Arguments:
- acts_in: bfloat16 [8192, 512], P('rep')
- w_first: bfloat16 [1024, 512], P(('rep', 'model'))
- w_middle: bfloat16 [1024, 1024], P(('rep', 'model'))
- w_last: bfloat16 [1024, 1024], P(('rep', 'model'))
- u_first: float32 [1024], P(('rep', 'model'))
- u_middle: float32 [1024], P(('rep', 'model'))
- u_last: float32 [1024], P(('rep', 'model'))
- target: bfloat16 [8192, 1024], P('rep', 'model')
Outputs:
- output 1: float32 [1], P('rep')
- output 2: bfloat16 [8192, 512], P('rep')
- output 3: float32 [1024, 512], P(('rep', 'model'))
- output 4: float32 [1024, 1024], P(('rep', 'model'))
- output 5: float32 [1024, 1024], P(('rep', 'model'))
- output 6: float32 [1024], P(('rep', 'model'))
- output 7: float32 [1024], P(('rep', 'model'))
- output 8: float32 [1024], P(('rep', 'model'))
- output 9: bfloat16 [512], P('rep')
- output 10: bfloat16 [1024], P('rep')
- output 11: bfloat16 [1024], P('rep')
- output 12: float32 [3], P('rep')
All inputs are finite; a program needn't handle non-finite values.
Results may differ from the reference program's by a relative error of at most 0.02.
Values are sent between devices in bfloat16 or wider.
A program may use at most 768 MiB of HBM per device.

```python
import functools
import math
import jax
import jax.numpy as jnp

D0 = 512
D1 = 1024
D2 = 1024
D3 = 1024
TOKENS = 8192
POWER_STEPS = 2

LEAK = 0.2
NORM_FLOOR = 1e-12


def spike_gain(rows_out, cols_in):
    return 1.5 * (1.0 + math.sqrt(rows_out / cols_in))


def unit_vector(vector):
    return vector / jnp.sqrt(jnp.sum(vector * vector))


def draw_layer(layer_key, rows_out, cols_in):
    key_left, key_right, key_bulk, key_start = jax.random.split(layer_key, 4)
    left_dir = unit_vector(jax.random.normal(key_left, (rows_out,), jnp.float32))
    right_dir = unit_vector(jax.random.normal(key_right, (cols_in,), jnp.float32))
    bulk_part = jax.random.normal(key_bulk, (rows_out, cols_in), jnp.float32) / math.sqrt(cols_in)
    weight = spike_gain(rows_out, cols_in) * jnp.outer(left_dir, right_dir) + bulk_part
    other_dir = jax.random.normal(key_start, (rows_out,), jnp.float32)
    other_dir = unit_vector(other_dir - jnp.dot(other_dir, left_dir) * left_dir)
    u_start = 0.6 * left_dir + 0.8 * other_dir
    return weight.astype(jnp.bfloat16), u_start


def setup_inputs(seed: int = 0, part: int = 0) -> dict:
    main_key = jax.random.fold_in(jax.random.key(seed), part)
    key_first, key_middle, key_last, key_acts, key_target = jax.random.split(main_key, 5)
    w_first, u_first = draw_layer(key_first, D1, D0)
    w_middle, u_middle = draw_layer(key_middle, D2, D1)
    w_last, u_last = draw_layer(key_last, D3, D2)
    act_gain = 2.0 * spike_gain(D1, D0) * spike_gain(D2, D1) * spike_gain(D3, D2)
    acts_in = (act_gain * jax.random.normal(key_acts, (TOKENS, D0), jnp.float32)).astype(jnp.bfloat16)
    target = (0.6 * jax.random.normal(key_target, (TOKENS, D3), jnp.float32)).astype(jnp.bfloat16)
    return {"acts_in": acts_in, "w_first": w_first, "w_middle": w_middle, "w_last": w_last, "u_first": u_first, "u_middle": u_middle, "u_last": u_last, "target": target}


def power_steps(weight, u_vec):
    for step_index in range(POWER_STEPS):
        p_vec = jnp.dot(u_vec.astype(jnp.bfloat16), weight, preferred_element_type=jnp.float32)
        v_vec = (p_vec / jnp.maximum(jnp.sqrt(jnp.sum(p_vec * p_vec)), NORM_FLOOR)).astype(jnp.bfloat16)
        s_vec = jnp.dot(weight, v_vec, preferred_element_type=jnp.float32)
        sigma_val = jnp.sqrt(jnp.sum(s_vec * s_vec))
        u_vec = s_vec / sigma_val
    return u_vec, v_vec, sigma_val


def stack_loss(weights_wide, acts_in, target, u_news, v_news):
    layer_in = acts_in
    for layer in range(3):
        sigma_val = jnp.dot(u_news[layer], jnp.dot(weights_wide[layer], v_news[layer].astype(jnp.float32)))
        y_out = jnp.dot(layer_in.astype(jnp.float32), weights_wide[layer].T) / sigma_val
        if layer < 2:
            layer_in = jax.nn.leaky_relu(y_out, LEAK).astype(jnp.bfloat16)
    residual = y_out - target.astype(jnp.float32)
    return (0.5 / TOKENS) * jnp.sum(residual * residual)


def reference(acts_in, w_first, w_middle, w_last, u_first, u_middle, u_last, target):
    weights = (w_first, w_middle, w_last)
    powered = [power_steps(weight, u_vec) for weight, u_vec in zip(weights, (u_first, u_middle, u_last))]
    u_news = [entry[0] for entry in powered]
    v_news = [entry[1] for entry in powered]
    sigmas = jnp.stack([entry[2] for entry in powered])
    loss_fn = functools.partial(stack_loss, target=target, u_news=u_news, v_news=v_news)
    weights_wide = [weight.astype(jnp.float32) for weight in weights]
    loss_value, pullback = jax.vjp(loss_fn, weights_wide, acts_in)
    weight_grads, grad_in = pullback(jnp.ones_like(loss_value))
    return (loss_value.reshape(1), grad_in, weight_grads[0], weight_grads[1], weight_grads[2], u_news[0], u_news[1], u_news[2], v_news[0], v_news[1], v_news[2], sigmas)
```

```python
import jax
import jax.numpy as jnp
from jax import lax
from jax.sharding import PartitionSpec as P

LEAK = 0.2
NORM_FLOOR = 1e-12
POWER_STEPS = 2
ROW_DIMS = (((1,), (1,)), ((), ()))
BATCH_DIMS = (((0,), (0,)), ((), ()))


def power_steps(weight, u_vec):
    for step_index in range(POWER_STEPS):
        p_vec = jnp.dot(u_vec.astype(jnp.bfloat16), weight, preferred_element_type=jnp.float32)
        v_vec = (p_vec / jnp.maximum(jnp.sqrt(jnp.sum(p_vec * p_vec)), NORM_FLOOR)).astype(jnp.bfloat16)
        s_vec = jnp.dot(weight, v_vec, preferred_element_type=jnp.float32)
        sigma_val = jnp.sqrt(jnp.sum(s_vec * s_vec))
        u_vec = s_vec / sigma_val
    return u_vec, v_vec, sigma_val


def device_program(acts_in, w_first, w_middle, w_last, u_first, u_middle, u_last, target):
    n = lax.axis_size("model")
    me = lax.axis_index("model")
    row_count = acts_in.shape[0]
    rows = row_count // n
    weights = [lax.all_gather(w, "model", axis=0, tiled=True) for w in (w_first, w_middle, w_last)]
    u_rows = u_first.shape[0]
    u_all = lax.all_gather(jnp.stack([u_first, u_middle, u_last]), "model", axis=1, tiled=True)
    target_rows = lax.all_to_all(target, "model", split_axis=0, concat_axis=1, tiled=True)
    layer_in = [lax.dynamic_slice_in_dim(acts_in, me * rows, rows, 0)]
    layer_out = []
    powered = []
    for layer in range(3):
        powered.append(power_steps(weights[layer], u_all[layer]))
        y_local = lax.dot_general(layer_in[layer], weights[layer], ROW_DIMS, preferred_element_type=jnp.float32) / powered[layer][2]
        layer_out.append(y_local)
        if layer < 2:
            layer_in.append(jax.nn.leaky_relu(y_local, LEAK).astype(jnp.bfloat16))
    residual = layer_out[2] - target_rows.astype(jnp.float32)
    loss_value = lax.psum(jnp.sum(residual * residual), "model") * (0.5 / row_count)
    grad_y = residual / row_count
    weight_grads = [None, None, None]
    grad_in = None
    for layer in (2, 1, 0):
        u_new, v_vec, sigma_val = powered[layer]
        grad_low = grad_y.astype(jnp.bfloat16)
        grad_mat = lax.dot_general(grad_low, layer_in[layer], BATCH_DIMS, preferred_element_type=jnp.float32)
        corr_sum = jnp.sum(grad_y * layer_out[layer])
        share = (grad_mat - corr_sum * jnp.outer(u_new, v_vec.astype(jnp.float32))) / sigma_val
        weight_grads[layer] = lax.psum_scatter(share, "model", scatter_dimension=0, tiled=True)
        grad_act = (jnp.dot(grad_low, weights[layer], preferred_element_type=jnp.float32) / sigma_val).astype(jnp.bfloat16)
        if layer > 0:
            grad_y = grad_act.astype(jnp.float32) * jnp.where(layer_out[layer - 1] >= 0, 1.0, LEAK)
        else:
            grad_in = lax.all_gather(grad_act, "model", axis=0, tiled=True)
    sigmas = jnp.stack([powered[0][2], powered[1][2], powered[2][2]])
    u_next = [lax.dynamic_slice_in_dim(entry[0], me * u_rows, u_rows, 0) for entry in powered]
    return (loss_value.reshape(1), grad_in, weight_grads[0], weight_grads[1], weight_grads[2], u_next[0], u_next[1], u_next[2], powered[0][1], powered[1][1], powered[2][1], sigmas)


def solution(mesh):
    row_spec = P("rep", None)
    weight_spec = P(("rep", "model"), None)
    vector_spec = P(("rep", "model"))
    group_spec = P("rep")
    in_specs = (row_spec, weight_spec, weight_spec, weight_spec, vector_spec, vector_spec, vector_spec, P("rep", "model"))
    out_specs = (group_spec, row_spec, weight_spec, weight_spec, weight_spec, vector_spec, vector_spec, vector_spec, group_spec, group_spec, group_spec, group_spec)
    return jax.shard_map(device_program, mesh=mesh, in_specs=in_specs, out_specs=out_specs, check_vma=False)
```

```python
import math

import jax
import jax.numpy as jnp
from jax import lax
from jax.experimental import pallas as pl
from jax.experimental.pallas import tpu as pltpu
from jax.sharding import PartitionSpec as P

LEAK = 0.2
NORM_FLOOR = 1e-12
POWER_STEPS = 2
MESH = pl.DeviceIdType.MESH
F32 = jnp.float32
BF16 = jnp.bfloat16
NN = (((1,), (0,)), ((), ()))
NT = (((1,), (1,)), ((), ()))
TN = (((0,), (0,)), ((), ()))
CORES = 2
LANES = 128
SUB = 16
TILE = 256
AG_SEMS = 72
RS_SEMS = 20
TG_SEMS = 28
DX_PARTS = 2
XP, XM, YP, YM = (1, 0), (-1, 0), (0, 1), (0, -1)


def dot(lhs, rhs, dims):
    return lax.dot_general(lhs, rhs, dims, preferred_element_type=F32)


class Place:
    def __init__(self, n):
        self.side = math.isqrt(n // CORES)
        me = lax.axis_index("model")
        self.me = me
        self.core = lax.rem(me, CORES)
        self.x = lax.rem(me // CORES, self.side)
        self.y = me // (CORES * self.side)

    def col(self, dx):
        return lax.rem(self.x + (dx + self.side), self.side)

    def row(self, dy):
        return lax.rem(self.y + (dy + self.side), self.side)

    def dev(self, rel, other=False):
        core = 1 - self.core if other else self.core
        return (self.row(rel[1]) * self.side + self.col(rel[0])) * CORES + core

    def norm(self, rel):
        s = self.side
        half = s // 2
        return tuple((r + half - 1) % s - (half - 1) for r in rel)


class Chan:
    def __init__(self, place, send_sems, recv_sems):
        self.place, self.send_sems, self.recv_sems = place, send_sems, recv_sems
        self.index, self.sent = {}, []

    def copy(self, key, src, dst, target):
        i = self.index.setdefault(key, len(self.index))
        return pltpu.make_async_remote_copy(
            src_ref=src, dst_ref=dst, send_sem=self.send_sems.at[i], recv_sem=self.recv_sems.at[i],
            device_id={"model": target}, device_id_type=MESH)

    def start(self, key, src, dst, target):
        desc = self.copy(key, src, dst, target)
        desc.start()
        self.sent.append(desc)

    def wait(self, key, dst):
        self.copy(key, dst, dst, self.place.dev((0, 0), True)).wait_recv()

    def drain(self):
        for desc in self.sent:
            desc.wait_send()
        self.sent = []


class Gather:
    def __init__(self, chan, ref_at, cuts, pair=True):
        self.chan, self.ref_at, self.pair = chan, ref_at, pair
        self.place = chan.place
        a, b, c, d, e = cuts
        keep = lambda *spans: [s for s in spans if s[1] > s[0]]
        self.full, self.mid, self.outer = keep((a, e)), keep((b, d)), keep((a, b), (d, e))
        self.half = {"x": keep((a, c)), "y": keep((c, e))}
        self.fwd = {"x": keep((b, c)), "y": keep((c, d))}
        self.bwd = {"x": keep((a, b)), "y": keep((d, e))}

    def start(self, rel, spans, way):
        rel = self.place.norm(rel)
        for s in spans:
            ref = self.ref_at(self.place.dev(rel), s)
            self.chan.start((rel, s, way), ref, ref, self.place.dev(way))

    def wait(self, rel, spans, way):
        rel = self.place.norm(rel)
        src = self.place.norm((rel[0] + way[0], rel[1] + way[1]))
        src = self.place.norm((rel[0] + way[0], rel[1] + way[1]))
        for s in spans:
            self.chan.wait((src, s, way), self.ref_at(self.place.dev(rel), s))

    def mate(self, *rels):
        if self.pair:
            for rel in rels:
                ref = self.ref_at(self.place.dev(rel), self.full[0])
                self.chan.start((rel, "mate"), ref, ref, self.place.dev((0, 0), True))

    def both(self, rel, spans, axis):
        for way in ((XP, XM) if axis == "x" else (YP, YM)):
            self.start(rel, spans, way)

    def step0(self):
        for way in (XP, XM, YP, YM):
            self.start((0, 0), self.full, way)
        self.mate((0, 0))

    def step1(self):
        for way in (XP, YP, XM, YM):
            rel = (-way[0], -way[1])
            self.wait(rel, self.full, way)
            self.start(rel, self.mid if way in (XP, YP) else self.outer, way)
            if way[0]:
                self.both(rel, self.half["x"], "y")
            else:
                self.both(rel, self.half["y"], "x")
            self.mate(rel)

    def hop(self, rel, axis):
        first = "x" if axis == "y" else "y"
        off = rel[1] if axis == "y" else rel[0]
        way = {("y", -1): YP, ("y", 1): YM, ("x", -1): XP, ("x", 1): XM}[(axis, off)]
        self.wait(rel, self.half[first], way)
        self.start(rel, (self.fwd if off < 0 else self.bwd)[first], way)

    def end(self, rel, axis):
        first = "x" if axis == "y" else "y"
        self.wait(rel, self.fwd[first], YP if axis == "y" else XP)
        self.wait(rel, self.bwd[first], YM if axis == "y" else XM)

    def step2(self):
        for d in (-1, 1):
            for e in (-1, 1):
                self.hop((d, e), "y")
                self.hop((e, d), "x")
        self.mate((-1, -1), (-1, 1), (1, -1), (1, 1))
        self.wait((2, 0), self.mid, XP)
        self.wait((2, 0), self.outer, XM)
        self.both((2, 0), self.half["x"], "y")
        self.wait((0, 2), self.mid, YP)
        self.wait((0, 2), self.outer, YM)
        self.both((0, 2), self.half["y"], "x")
        self.mate((2, 0), (0, 2))

    def step3(self):
        for d in (-1, 1):
            self.hop((2, d), "y")
            self.hop((d, 2), "x")
        for d in (-1, 1):
            self.end((d, 2), "y")
            self.end((2, d), "x")
        self.mate((-1, 2), (1, 2), (2, -1), (2, 1))

    def step4(self):
        self.end((2, 2), "y")
        self.end((2, 2), "x")
        self.mate((2, 2))

    def finish(self):
        if self.pair:
            r = range(-1, self.place.side - 1)
            for rel in [(dx, dy) for dx in r for dy in r]:
                self.chan.wait((rel, "mate"), self.ref_at(self.place.dev(rel, True), self.full[0]))


class Reduce:
    def __init__(self, chan, blocks, mate, relay, main, relay2, main2, acc, width):
        self.chan, self.place = chan, chan.place
        self.blocks, self.mate = blocks, mate
        self.relay, self.main, self.relay2, self.main2, self.acc = relay, main, relay2, main2, acc
        q = width // 4
        self.q = q
        self.cols = {"x": ((q, 2 * q), (0, q), (0, 2 * q)), "y": ((2 * q, 3 * q), (3 * q, 4 * q), (2 * q, 4 * q))}

    def at(self, axis, pos, span):
        cols = pl.ds(span[0], span[1] - span[0])
        if axis == "x":
            return self.blocks.at[:, pos, self.place.core, :, cols]
        return self.blocks.at[pos, :, self.place.core, :, cols]

    def one(self, dx, dy, span):
        return self.blocks.at[self.place.row(dy), self.place.col(dx), self.place.core, :, pl.ds(span[0], span[1] - span[0])]

    def pair_send(self):
        p = self.place
        self.chan.start("pair", self.blocks.at[:, :, 1 - p.core], self.mate, p.dev((0, 0), True))

    def pair_add(self):
        p = self.place
        self.chan.wait("pair", self.mate)
        for k in range(p.side):
            mine = self.blocks.at[k, :, p.core]
            mine[...] = (mine[...].astype(F32) + self.mate[k].astype(F32)).astype(BF16)

    def pos(self, axis, d):
        return self.place.col(d) if axis == "x" else self.place.row(d)

    def ways(self, axis):
        return (XP, XM) if axis == "x" else (YP, YM)

    def far_send(self):
        for h, axis in enumerate(("x", "y")):
            for s, way in enumerate(self.ways(axis)):
                self.chan.start(("far", h, s), self.at(axis, self.pos(axis, 2), self.cols[axis][s]),
                                self.relay.at[h, s], self.place.dev(way))

    def far_add(self):
        for h, axis in enumerate(("x", "y")):
            for s, way in enumerate(self.ways(axis)):
                self.chan.wait(("far", h, s), self.relay.at[h, s])
                step = 1 if s == 0 else -1
                ref = self.at(axis, self.pos(axis, step), self.cols[axis][s])
                ref[...] = (ref[...].astype(F32) + self.relay[h, s].astype(F32)).astype(BF16)
                self.chan.start(("near", h, s), self.at(axis, self.pos(axis, step), self.cols[axis][2]),
                                self.main.at[h, s], self.place.dev(way))

    def near_add(self):
        p = self.place
        for h, (axis, cross) in enumerate((("x", "y"), ("y", "x"))):
            for s in range(2):
                self.chan.wait(("near", h, s), self.main.at[h, s])
            own = self.pos(cross, 0)
            span = self.cols[axis][2]
            self.acc[h] = (self.one(0, 0, span)[...].astype(F32) + self.main[h, 0, own].astype(F32)
                           + self.main[h, 1, own].astype(F32))
            ref = self.at(axis, self.pos(axis, 0), span)
            ref[...] = (ref[...].astype(F32) + self.main[h, 0].astype(F32) + self.main[h, 1].astype(F32)).astype(BF16)
            for s, way in enumerate(self.ways(cross)):
                d = (0, 2) if cross == "y" else (2, 0)
                self.chan.start(("far2", h, s), self.one(d[0], d[1], self.cols[axis][s]),
                                self.relay2.at[h, s], p.dev(way))

    def far2_add(self):
        p = self.place
        for h, (axis, cross) in enumerate((("x", "y"), ("y", "x"))):
            for s, way in enumerate(self.ways(cross)):
                self.chan.wait(("far2", h, s), self.relay2.at[h, s])
                ref = self.one(way[0], way[1], self.cols[axis][s])
                ref[...] = (ref[...].astype(F32) + self.relay2[h, s].astype(F32)).astype(BF16)
                self.chan.start(("near2", h, s), self.one(way[0], way[1], self.cols[axis][2]),
                                self.main2.at[h, s], p.dev(way))

    def finish(self, out_ref, inv):
        for h in range(2):
            for s in range(2):
                self.chan.wait(("near2", h, s), self.main2.at[h, s])
            out_ref[:, pl.ds(2 * self.q * h, 2 * self.q)] = (
                self.acc[h] + self.main2[h, 0].astype(F32) + self.main2[h, 1].astype(F32)) * inv


class Spread:
    def __init__(self, chan, mine, stage, relay, mid, final):
        self.chan, self.place = chan, chan.place
        self.mine, self.stage, self.relay, self.mid, self.final = mine, stage, relay, mid, final

    def pair_send(self):
        p = self.place
        self.chan.start("pair", self.mine.at[1 - p.core], self.stage.at[p.core], p.dev((0, 0), True))

    def pair_take(self):
        p = self.place
        self.stage[p.core] = self.mine[p.core]
        self.chan.wait("pair", self.stage.at[1 - p.core])

    def src(self, h, pos, lo, hi):
        rest = pl.ds(lo, hi - lo)
        return self.stage.at[h, rest, pos] if h == 0 else self.stage.at[h, pos, rest]

    def first_send(self):
        p = self.place
        s2 = p.side // 2
        for h in range(2):
            here = p.x if h == 0 else p.y
            ways = (XP, XM) if h == 0 else (YP, YM)
            pos = p.col if h == 0 else p.row
            for s, way in enumerate(ways):
                self.chan.start(("far", h, s), self.src(h, pos(2), s * s2, s * s2 + s2), self.relay.at[h, s], p.dev(way))
            for s, way in enumerate(ways):
                d = 1 if s == 0 else -1
                self.chan.start(("near", h, s), self.src(h, pos(d), 0, p.side), self.mid.at[h, here], p.dev(way))
            self.mid[h, here] = self.src(h, here, 0, p.side)[...]

    def first_relay(self):
        p = self.place
        s2 = p.side // 2
        for h in range(2):
            ways = (XP, XM) if h == 0 else (YP, YM)
            pos = p.col if h == 0 else p.row
            for s, way in enumerate(ways):
                self.chan.wait(("far", h, s), self.relay.at[h, s])
                self.chan.start(("on", h, s), self.relay.at[h, s],
                                self.mid.at[h, pos(-1 if s == 0 else 1), pl.ds(s * s2, s2)], p.dev(way))

    def second_send(self):
        p = self.place
        s2 = p.side // 2
        for h in range(2):
            pos = p.col if h == 0 else p.row
            for s in range(2):
                self.chan.wait(("near", h, s), self.mid.at[h, pos(-1 if s == 0 else 1)])
                self.chan.wait(("on", h, s), self.mid.at[h, pos(2), pl.ds(s * s2, s2)])
            cross = p.row if h == 0 else p.col
            ways = (YP, YM) if h == 0 else (XP, XM)
            for s, way in enumerate(ways):
                self.chan.start(("far2", h, s), self.mid.at[h, pl.ds(s * s2, s2), cross(2)],
                                self.relay.at[2 + h, s], p.dev(way))
            for s, way in enumerate(ways):
                self.chan.start(("near2", h, s), self.mid.at[h, :, cross(1 if s == 0 else -1)],
                                self.dst(h, cross(0), 0, p.side), p.dev(way))
            self.dst(h, cross(0), 0, p.side)[...] = self.mid[h, :, cross(0)]

    def dst(self, h, pos, lo, hi):
        rest = pl.ds(lo, hi - lo)
        return self.final.at[pos, rest, h] if h == 0 else self.final.at[rest, pos, h]

    def second_relay(self):
        p = self.place
        s2 = p.side // 2
        for h in range(2):
            cross = p.row if h == 0 else p.col
            ways = (YP, YM) if h == 0 else (XP, XM)
            for s, way in enumerate(ways):
                self.chan.wait(("far2", h, s), self.relay.at[2 + h, s])
                self.chan.start(("on2", h, s), self.relay.at[2 + h, s],
                                self.dst(h, cross(-1 if s == 0 else 1), s * s2, s * s2 + s2), p.dev(way))

    def finish(self):
        p = self.place
        s2 = p.side // 2
        for h in range(2):
            cross = p.row if h == 0 else p.col
            for s in range(2):
                self.chan.wait(("near2", h, s), self.dst(h, cross(-1 if s == 0 else 1), 0, p.side))
                self.chan.wait(("on2", h, s), self.dst(h, cross(2), s * s2, s * s2 + s2))


def row_of(value, rows):
    return jnp.broadcast_to(value, (rows, value.shape[1]))


def split3(value):
    hi = value.astype(BF16)
    rest = value - hi.astype(F32)
    mid = rest.astype(BF16)
    lo = (rest - mid.astype(F32)).astype(BF16)
    return hi, mid, lo


def kernel(n, acts_hbm, w0_hbm, w1_hbm, w2_hbm, u0_ref, u1_ref, u2_ref, target_hbm,
           loss_ref, dx_ref, g0_ref, g1_ref, g2_ref, un0_ref, un1_ref, un2_ref, v0_ref, v1_ref, v2_ref, sig_ref,
           w0, w1, w2, x0, x1, x2, y0, y1, y2, grad, low, sq,
           tbuf, tmine, tstage, trelay, tmid, tfinal, lossbuf, losspair,
           d0, d1, d2, m0, m1, m2,
           ra0, rb0, rc0, re0, rf0, ra1, rb1, rc1, re1, rf1, ra2, rb2, rc2, re2, rf2,
           local_sems, w_send, w_recv, dx_send, dx_recv, rs_send, rs_recv, t_send, t_recv, l_send, l_recv):
    p = Place(n)
    side = p.side
    rows = x0.shape[0]
    wr = w0_hbm.shape[0]
    total_rows = dx_ref.shape[0]
    k0 = w0_hbm.shape[1]
    k1 = w1_hbm.shape[1]
    mine = pl.ds(pl.multiple_of(p.me * wr, wr), wr)

    loads = [
        pltpu.make_async_copy(w0_hbm, w0.at[mine, pl.ds(0, k0)], local_sems.at[0]),
        pltpu.make_async_copy(w1_hbm, w1.at[mine], local_sems.at[1]),
        pltpu.make_async_copy(w2_hbm, w2.at[mine], local_sems.at[2]),
        pltpu.make_async_copy(target_hbm, tbuf, local_sems.at[3]),
        pltpu.make_async_copy(acts_hbm.at[pl.ds(pl.multiple_of(p.me * rows, rows), rows)], x0, local_sems.at[4]),
    ]
    for load in loads:
        load.start()

    barrier = pltpu.get_barrier_semaphore()
    peers = [p.dev(way) for way in (XP, XM, YP, YM)] + [p.dev((0, 0), True)]
    for peer in peers:
        pl.semaphore_signal(barrier, inc=1, device_id={"model": peer}, device_id_type=MESH)

    lane = lax.broadcasted_iota(jnp.int32, (wr, LANES), 1)
    eye = (lax.broadcasted_iota(jnp.int32, (wr, wr), 0) == lax.broadcasted_iota(jnp.int32, (wr, wr), 1))
    uext = jnp.zeros((wr, LANES), F32)
    for i, ref in enumerate((u0_ref, u1_ref, u2_ref)):
        column = jnp.sum(jnp.where(eye, jnp.broadcast_to(ref[...], (wr, wr)), 0.0), axis=1, keepdims=True)
        uext = jnp.where(lane == i, column, uext)
    w0[mine, pl.ds(k0, LANES)] = uext.astype(BF16)

    pl.semaphore_wait(barrier, len(peers))

    def weight_at(ref):
        return lambda dev, s: ref.at[pl.ds(pl.multiple_of(dev * wr, wr), wr), pl.ds(s[0], s[1] - s[0])]

    q = k1 // 4
    wide = k0 + LANES
    gathers = []
    for i, (ref, cuts) in enumerate(((w0, (0, LANES, 3 * LANES, 4 * LANES, wide)), (w1, (0, q, 2 * q, 3 * q, k1)), (w2, (0, q, 2 * q, 3 * q, k1)))):
        gathers.append(Gather(Chan(p, w_send.at[i], w_recv.at[i]), weight_at(ref), cuts))
    ga, gb, gc = gathers
    for i, g in enumerate(gathers):
        loads[i].wait()
        g.step0()

    loads[3].wait()
    eye32 = eye.astype(BF16)
    cols = tbuf.shape[1]

    def turn(j, carry):
        piece = dot(eye32, tbuf[pl.ds(pl.multiple_of(j * rows, rows), rows), :], NT).astype(BF16)
        chip = j // CORES
        tmine[lax.rem(j, CORES), chip // side, lax.rem(chip, side)] = piece
        return carry

    lax.fori_loop(0, n, turn, 0)
    spread = Spread(Chan(p, t_send, t_recv), tmine, tstage, trelay, tmid, tfinal)
    spread.pair_send()
    ga.step1()
    gb.step1()
    spread.pair_take()
    gc.step1()
    spread.first_send()
    ga.step2()
    gb.step2()
    spread.first_relay()
    gc.step2()
    ga.step3()
    ga.step4()
    ga.finish()

    def matvec(vec, ref, dims, width):
        return dot(vec, ref[:, pl.ds(0, width)], dims)

    def power(i, w_ref, width, u16):
        for step in range(POWER_STEPS):
            pv = matvec(u16.astype(BF16), w_ref, NN, width)
            norm = jnp.sqrt(jnp.sum(pv * pv, axis=1, keepdims=True))
            v16 = (pv / jnp.maximum(norm, NORM_FLOOR)).astype(BF16)
            sv = matvec(v16, w_ref, NT, width)
            sigma = jnp.sqrt(jnp.sum(sv * sv, axis=1, keepdims=True))
            u16 = sv / sigma
        own = dot(v16, w_ref[mine, pl.ds(0, width)], NT) / sigma
        (un0_ref, un1_ref, un2_ref)[i][...] = own[0:1]
        (v0_ref, v1_ref, v2_ref)[i][...] = v16[0:1]
        return u16, v16, sigma[0:1, 0:1]

    def u_start(i):
        picked = (lax.broadcasted_iota(jnp.int32, (SUB, LANES), 1) == i).astype(BF16)
        return dot(picked, w0[:, pl.ds(k0, LANES)], NT)

    def forward(x_ref, w_ref, width, inv, y_ref, next_ref):
        def body(j, carry):
            at = pl.ds(pl.multiple_of(j * TILE, TILE), TILE)
            y = dot(x_ref[...], w_ref[at, pl.ds(0, width)], NT) * inv
            y_ref[:, at] = y
            if next_ref is not None:
                next_ref[:, at] = jnp.where(y >= 0, y, LEAK * y).astype(BF16)
            return carry

        lax.fori_loop(0, y_ref.shape[1] // TILE, body, 0)

    loads[4].wait()
    u16a, v16a, sa = power(0, w0, k0, u_start(0))
    inva = 1.0 / sa
    forward(x0, w0, k0, inva, y0, x1)
    gb.step3()
    gb.step4()
    spread.second_send()
    gc.step3()
    gb.finish()
    u16b, v16b, sb = power(1, w1, k1, u_start(1))
    invb = 1.0 / sb
    gc.step4()
    spread.second_relay()
    forward(x1, w1, k1, invb, y1, x2)
    gc.finish()
    u16c, v16c, sc = power(2, w2, k1, u_start(2))
    invc = 1.0 / sc
    forward(x2, w2, k1, invc, y2, None)
    spread.finish()

    lane1 = lax.broadcasted_iota(jnp.int32, (1, LANES), 1)
    sig_ref[...] = jnp.where(lane1 == 0, sa, jnp.where(lane1 == 1, sb, sc))

    scale = 1.0 / total_rows
    eyer = (lax.broadcasted_iota(jnp.int32, (rows, rows), 0) == lax.broadcasted_iota(jnp.int32, (rows, rows), 1)).astype(BF16)
    zero11 = jnp.zeros((1, 1), F32)

    def total(value):
        return jnp.sum(jnp.sum(value, axis=0, keepdims=True), axis=1, keepdims=True)

    loss = zero11
    corr = zero11
    span = TILE // (CORES * wr)
    for j in range(y2.shape[1] // TILE):
        at = pl.ds(j * TILE, TILE)
        block = tfinal[j * span // side] if span == side else None
        t = dot(eyer, block.reshape(TILE, rows), NT)
        residual = y2[:, at] - t
        g = residual * scale
        grad[:, at] = g
        low[:, at] = g.astype(BF16)
        loss = loss + total(residual * residual)
        corr = corr + total(g * y2[:, at])

    lossbuf[p.dev((0, 0)) // CORES] = jnp.broadcast_to(loss, lossbuf.shape[1:])
    lchan = Chan(p, l_send, l_recv)
    losspair[0] = jnp.broadcast_to(loss, losspair.shape[1:])
    lchan.start("pair", losspair.at[0], losspair.at[1], p.dev((0, 0), True))

    def share(x_ref, d_ref, width, corr, u16, v16):
        minus = [row_of(part[0:1], 1) for part in split3(u16[0:1] * (-corr))]
        sub = lax.broadcasted_iota(jnp.int32, (SUB, u16.shape[1]), 0)
        uu = jnp.zeros(sub.shape, F32)
        for i, part in enumerate(minus):
            uu = jnp.where(sub == i, jnp.broadcast_to(part.astype(F32), sub.shape), uu)
        sq[...] = uu.astype(BF16)

        def body(j, carry):
            at = pl.ds(pl.multiple_of(j * TILE, TILE), TILE)
            full = dot(low[:, at], x_ref[...], TN) + dot(sq[:, at], v16, TN)
            d_ref[j] = full.astype(BF16).reshape(side, CORES, wr, width)
            return carry

        lax.fori_loop(0, side, body, 0)

    def back(w_ref, width, inv, y_ref):
        corr = zero11
        for j in range(width // TILE):
            at = pl.ds(j * TILE, TILE)
            dx = (dot(low[...], w_ref[:, at], NN) * inv).astype(BF16)
            y = y_ref[:, at]
            g = dx.astype(F32) * jnp.where(y >= 0, 1.0, LEAK)
            grad[:, at] = g
            corr = corr + total(g * y)
        return corr

    def lower():
        low[...] = grad[...].astype(BF16)

    def reducer(i, blocks, mate, relay, main, relay2, main2, acc, width):
        return Reduce(Chan(p, rs_send.at[i], rs_recv.at[i]), blocks, mate, relay, main, relay2, main2, acc, width)

    rc = reducer(2, d2, m2, ra2, rb2, rc2, re2, rf2, k1)
    rb = reducer(1, d1, m1, ra1, rb1, rc1, re1, rf1, k1)
    ra = reducer(0, d0, m0, ra0, rb0, rc0, re0, rf0, k0)
    share(x2, d2, k1, corr, u16c, v16c)
    rc.pair_send()
    corr = back(w2, k1, invc, y1)
    lower()
    rc.pair_add()
    rc.far_send()
    share(x1, d1, k1, corr, u16b, v16b)
    rb.pair_send()
    corr = back(w1, k1, invb, y0)
    lower()
    rc.far_add()
    rb.pair_add()
    rb.far_send()

    out_rows = pl.ds(pl.multiple_of(p.me * rows, rows), rows)
    for j in range(k0 // TILE):
        at = pl.ds(j * TILE, TILE)
        dx_ref[out_rows, at] = (dot(low[...], w0[:, at], NN) * inva).astype(BF16)
    share(x0, d0, k0, corr, u16a, v16a)
    ra.pair_send()

    part = rows // DX_PARTS
    gd = []
    for i in range(DX_PARTS):
        def dx_at(dev, s, i=i):
            return dx_ref.at[pl.ds(pl.multiple_of(dev * rows + (i * part + s[0]), 16), s[1] - s[0])]

        gd.append(Gather(Chan(p, dx_send.at[i], dx_recv.at[i]), dx_at, [part * k // 4 for k in range(5)]))
    for g in gd:
        g.step0()

    lchan.wait("pair", losspair.at[1])
    here = p.dev((0, 0)) // CORES
    lossbuf[here] = losspair[0] + losspair[1]
    lg = Gather(lchan, lambda dev, s: lossbuf.at[dev // CORES], (0, 0, 1, 1, 1), pair=False)

    ra.pair_add()
    rc.near_add()
    rb.far_add()
    ra.far_send()
    lg.step0()
    gd[0].step1()
    rc.far2_add()
    rb.near_add()
    ra.far_add()
    lg.step1()
    gd[1].step1()
    rc.finish(g2_ref, invc)
    rb.far2_add()
    ra.near_add()
    lg.step2()
    gd[0].step2()
    rb.finish(g1_ref, invb)
    ra.far2_add()
    lg.step3()
    gd[1].step2()
    ra.finish(g0_ref, inva)
    lg.step4()
    gd[0].step3()
    gd[1].step3()
    gd[0].step4()
    gd[1].step4()
    whole = jnp.zeros(losspair.shape[1:], F32)
    for k in range(n // CORES):
        whole = whole + lossbuf[k]
    loss_ref[...] = whole[0:1, 0:1] * (0.5 * scale)
    gd[0].finish()
    gd[1].finish()
    for chan in [g.chan for g in gathers] + [spread.chan, lchan, ra.chan, rb.chan, rc.chan] + [g.chan for g in gd]:
        chan.drain()


def device_program(n, acts_in, w_first, w_middle, w_last, u_first, u_middle, u_last, target):
    side = math.isqrt(n // CORES)
    total_rows, k0 = acts_in.shape
    rows = total_rows // n
    wr, k1 = w_middle.shape
    width = wr * n
    tcols = target.shape[1]
    chips = side * side

    def reduce_bufs(k):
        q = k // 4
        return [pltpu.VMEM((2, 2, side, wr, q), BF16), pltpu.VMEM((2, 2, side, wr, 2 * q), BF16),
                pltpu.VMEM((2, 2, wr, q), BF16), pltpu.VMEM((2, 2, wr, 2 * q), BF16), pltpu.VMEM((2, wr, 2 * q), F32)]

    vmem = pl.BlockSpec(memory_space=pltpu.VMEM)
    anym = pl.BlockSpec(memory_space=pl.ANY)
    out_shape = (
        jax.ShapeDtypeStruct((1, 1), F32), jax.ShapeDtypeStruct((total_rows, k0), BF16),
        jax.ShapeDtypeStruct((wr, k0), F32), jax.ShapeDtypeStruct((wr, k1), F32), jax.ShapeDtypeStruct((wr, k1), F32),
        jax.ShapeDtypeStruct((1, wr), F32), jax.ShapeDtypeStruct((1, wr), F32), jax.ShapeDtypeStruct((1, wr), F32),
        jax.ShapeDtypeStruct((1, k0), BF16), jax.ShapeDtypeStruct((1, k1), BF16), jax.ShapeDtypeStruct((1, k1), BF16),
        jax.ShapeDtypeStruct((1, LANES), F32))
    scratch = [
        pltpu.VMEM((width, k0 + LANES), BF16), pltpu.VMEM((width, k1), BF16), pltpu.VMEM((width, k1), BF16),
        pltpu.VMEM((rows, k0), BF16), pltpu.VMEM((rows, k1), BF16), pltpu.VMEM((rows, k1), BF16),
        pltpu.VMEM((rows, width), F32), pltpu.VMEM((rows, width), F32), pltpu.VMEM((rows, width), F32),
        pltpu.VMEM((rows, width), F32), pltpu.VMEM((rows, width), BF16), pltpu.VMEM((SUB, width), BF16),
        pltpu.VMEM((total_rows, tcols), BF16),
        pltpu.VMEM((CORES, side, side, tcols, rows), BF16), pltpu.VMEM((CORES, side, side, tcols, rows), BF16),
        pltpu.VMEM((4, 2, side // 2, tcols, rows), BF16), pltpu.VMEM((2, side, side, tcols, rows), BF16),
        pltpu.VMEM((side, side, CORES, tcols, rows), BF16),
        pltpu.VMEM((chips, 8, LANES), F32), pltpu.VMEM((2, 8, LANES), F32),
        pltpu.VMEM((side, side, CORES, wr, k0), BF16), pltpu.VMEM((side, side, CORES, wr, k1), BF16), pltpu.VMEM((side, side, CORES, wr, k1), BF16),
        pltpu.VMEM((side, side, wr, k0), BF16), pltpu.VMEM((side, side, wr, k1), BF16), pltpu.VMEM((side, side, wr, k1), BF16),
        *reduce_bufs(k0), *reduce_bufs(k1), *reduce_bufs(k1),
        pltpu.SemaphoreType.DMA((5,)),
        pltpu.SemaphoreType.DMA((3, AG_SEMS)), pltpu.SemaphoreType.DMA((3, AG_SEMS)),
        pltpu.SemaphoreType.DMA((DX_PARTS, AG_SEMS)), pltpu.SemaphoreType.DMA((DX_PARTS, AG_SEMS)),
        pltpu.SemaphoreType.DMA((3, RS_SEMS)), pltpu.SemaphoreType.DMA((3, RS_SEMS)),
        pltpu.SemaphoreType.DMA((TG_SEMS,)), pltpu.SemaphoreType.DMA((TG_SEMS,)),
        pltpu.SemaphoreType.DMA((AG_SEMS,)), pltpu.SemaphoreType.DMA((AG_SEMS,)),
    ]
    import functools
    outs = pl.pallas_call(
        functools.partial(kernel, n),
        out_shape=out_shape,
        in_specs=[anym, anym, anym, anym, vmem, vmem, vmem, anym],
        out_specs=(vmem,) * len(out_shape),
        scratch_shapes=scratch,
        compiler_params=pltpu.CompilerParams(collective_id=0, has_side_effects=True, vmem_limit_bytes=50 * 1024 * 1024),
        name="stack",
    )(acts_in, w_first, w_middle, w_last, u_first.reshape(1, wr), u_middle.reshape(1, wr), u_last.reshape(1, wr), target)
    loss, dx, g0, g1, g2, un0, un1, un2, v0, v1, v2, sig = outs
    return (loss.reshape(1), dx, g0, g1, g2, un0.reshape(wr), un1.reshape(wr), un2.reshape(wr),
            v0.reshape(k0), v1.reshape(k1), v2.reshape(k1), sig[0, :3])


def solution(mesh):
    n = mesh.shape["model"]
    row_spec = P("rep", None)
    weight_spec = P(("rep", "model"), None)
    vector_spec = P(("rep", "model"))
    group_spec = P("rep")
    in_specs = (row_spec, weight_spec, weight_spec, weight_spec, vector_spec, vector_spec, vector_spec, P("rep", "model"))
    out_specs = (group_spec, row_spec, weight_spec, weight_spec, weight_spec, vector_spec, vector_spec, vector_spec, group_spec, group_spec, group_spec, group_spec)
    return jax.shard_map(lambda *args: device_program(n, *args), mesh=mesh, in_specs=in_specs, out_specs=out_specs, check_vma=False)
```

```python
import functools
import math

import jax
import jax.numpy as jnp
from jax import lax
from jax.experimental import pallas as pl
from jax.experimental.pallas import tpu as pltpu
from jax.sharding import PartitionSpec as P

LEAK = 0.2
NORM_FLOOR = 1e-12
POWER_STEPS = 2
MESH = pl.DeviceIdType.MESH
F32 = jnp.float32
BF16 = jnp.bfloat16
NN = (((1,), (0,)), ((), ()))
NT = (((1,), (1,)), ((), ()))
CORES = 2
LANES = 128
SUB = 16
TILE = 256
FTILE = 512
VMEM_LIMIT = 40 * 1024 * 1024
TAKE_LIMIT = 66338816
EMIT_LIMIT = 12 * 1024 * 1024
DX_PARTS = 2
XP, XM, YP, YM = (1, 0), (-1, 0), (0, 1), (0, -1)


def dot(lhs, rhs, dims):
    return lax.dot_general(lhs, rhs, dims, preferred_element_type=F32)


class Place:
    def __init__(self, n):
        self.side = math.isqrt(n // CORES)
        me = lax.axis_index("model")
        self.me = me
        self.core = lax.rem(me, CORES)
        self.x = lax.rem(me // CORES, self.side)
        self.y = me // (CORES * self.side)

    def col(self, dx):
        return lax.rem(self.x + (dx + self.side), self.side)

    def row(self, dy):
        return lax.rem(self.y + (dy + self.side), self.side)

    def dev(self, rel, other=False):
        core = 1 - self.core if other else self.core
        return (self.row(rel[1]) * self.side + self.col(rel[0])) * CORES + core

    def at(self, x, y):
        return (y * self.side + x) * CORES + self.core

    def norm(self, rel):
        s = self.side
        half = s // 2
        return tuple((r + half - 1) % s - (half - 1) for r in rel)


class Link:
    def __init__(self, place, send_sem, recv_sems):
        self.place, self.send_sem, self.recv_sems = place, send_sem, recv_sems

    def copy(self, i, src, dst, target, send_sem=None):
        return pltpu.make_async_remote_copy(
            src_ref=src, dst_ref=dst, send_sem=self.send_sem if send_sem is None else send_sem,
            recv_sem=self.recv_sems.at[i], device_id={"model": target}, device_id_type=MESH)

    def start(self, i, src, dst, target, send_sem=None):
        self.copy(i, src, dst, target, send_sem).start()

    def wait(self, i, dst):
        self.copy(i, dst, dst, self.place.dev((0, 0), True)).wait_recv()

    def drain(self, sent, send_sem=None):
        self.copy(0, sent, sent, self.place.dev((0, 0), True), send_sem).wait_send()


class Gather:
    def __init__(self, link, ref_at, bulk, cuts):
        self.link, self.ref_at, self.bulk, self.place = link, ref_at, bulk, link.place
        a, b, c, d, e = cuts
        self.full, self.mid, self.outer = ((a, e),), ((b, d),), ((a, b), (d, e))
        self.half = {"x": ((a, c),), "y": ((c, e),)}
        self.fwd = {"x": ((b, c),), "y": ((c, d),)}
        self.bwd = {"x": ((a, b),), "y": ((d, e),)}

    def number(self, rel):
        return (rel[1] + 1) * self.place.side + rel[0] + 1

    def start(self, rel, spans, way, src=None):
        there = self.number(self.place.norm((rel[0] - way[0], rel[1] - way[1])))
        for s in spans:
            ref = self.ref_at(self.place.dev(rel), s)
            self.link.start(there, ref if src is None else src, ref, self.place.dev(way))

    def take(self, rel):
        self.link.wait(self.number(rel), self.ref_at(self.place.dev(rel), self.full[0]))

    def mate(self, rel, src=None):
        ref = self.ref_at(self.place.dev(rel), self.full[0])
        self.link.start(self.number((0, 0)), ref if src is None else src, ref, self.place.dev((0, 0), True))

    def cross(self, rel, axis):
        for way in ((YP, YM) if axis == "x" else (XP, XM)):
            self.start(rel, self.half[axis], way)

    def relay(self, rel, axis, first):
        off = rel[0] if axis == "x" else rel[1]
        way = {("x", -1): XP, ("x", 1): XM, ("y", -1): YP, ("y", 1): YM}[(axis, off)]
        self.start(rel, (self.fwd if off < 0 else self.bwd)[first], way)

    def step0(self, src=None):
        for way in (XP, YP, XM, YM):
            self.start((0, 0), self.full, way, src)
        self.mate((0, 0), src)

    def step1(self):
        for way in (XP, YP, XM, YM):
            rel = (-way[0], -way[1])
            self.take(rel)
            self.start(rel, self.mid if way in (XP, YP) else self.outer, way)
            self.cross(rel, "x" if way[0] else "y")
            self.mate(rel)

    def step2(self):
        for rel, axis in (((2, 0), "x"), ((0, 2), "y")):
            self.take(rel)
            self.cross(rel, axis)
            self.mate(rel)
        for rel in ((-1, -1), (-1, 1), (1, -1), (1, 1)):
            self.take(rel)
            self.relay(rel, "y", "x")
            self.relay(rel, "x", "y")
            self.mate(rel)

    def step3(self):
        for d in (-1, 1):
            self.take((2, d))
            self.relay((2, d), "y", "x")
            self.mate((2, d))
            self.take((d, 2))
            self.relay((d, 2), "x", "y")
            self.mate((d, 2))

    def step4(self):
        self.take((2, 2))
        self.mate((2, 2))

    def finish(self):
        self.link.wait(self.number((0, 0)), self.bulk(self.place.side ** 2))

    def drain(self):
        self.link.drain(self.bulk(CORES * self.place.side ** 2 - 1))


class Reduce:
    def __init__(self, link, blocks, mate, relay, main, relay2, main2, acc, width):
        self.link, self.place = link, link.place
        self.blocks, self.mate = blocks, mate
        self.relay, self.main, self.relay2, self.main2, self.acc = relay, main, relay2, main2, acc
        q = width // 4
        self.q = q
        self.cols = {"x": ((q, 2 * q), (0, q), (0, 2 * q)), "y": ((2 * q, 3 * q), (3 * q, 4 * q), (2 * q, 4 * q))}

    def at(self, axis, pos, span):
        cols = pl.ds(span[0], span[1] - span[0])
        if axis == "x":
            return self.blocks.at[:, pos, self.place.core, :, cols]
        return self.blocks.at[pos, :, self.place.core, :, cols]

    def one(self, dx, dy, span):
        return self.blocks.at[self.place.row(dy), self.place.col(dx), self.place.core, :, pl.ds(span[0], span[1] - span[0])]

    def pair_send(self):
        p = self.place
        self.link.start(0, self.blocks.at[:, :, 1 - p.core], self.mate, p.dev((0, 0), True))

    def pair_add(self):
        p = self.place
        self.link.wait(0, self.mate)
        for k in range(p.side):
            mine = self.blocks.at[k, :, p.core]
            mine[...] = (mine[...].astype(F32) + self.mate[k].astype(F32)).astype(BF16)

    def pos(self, axis, d):
        return self.place.col(d) if axis == "x" else self.place.row(d)

    def ways(self, axis):
        return (XP, XM) if axis == "x" else (YP, YM)

    def far_send(self):
        for h, axis in enumerate(("x", "y")):
            for s, way in enumerate(self.ways(axis)):
                self.link.start(1 + 2 * h + s, self.at(axis, self.pos(axis, 2), self.cols[axis][s]),
                                self.relay.at[h, s], self.place.dev(way))

    def far_add(self):
        for h, axis in enumerate(("x", "y")):
            for s, way in enumerate(self.ways(axis)):
                self.link.wait(1 + 2 * h + s, self.relay.at[h, s])
                step = 1 if s == 0 else -1
                ref = self.at(axis, self.pos(axis, step), self.cols[axis][s])
                ref[...] = (ref[...].astype(F32) + self.relay[h, s].astype(F32)).astype(BF16)
                self.link.start(5 + h, self.at(axis, self.pos(axis, step), self.cols[axis][2]),
                                self.main.at[h, s], self.place.dev(way))

    def near_add(self):
        p = self.place
        for h, (axis, cross) in enumerate((("x", "y"), ("y", "x"))):
            self.link.wait(5 + h, self.main.at[h])
            own = self.pos(cross, 0)
            span = self.cols[axis][2]
            self.acc[h] = (self.one(0, 0, span)[...].astype(F32) + self.main[h, 0, own].astype(F32)
                           + self.main[h, 1, own].astype(F32))
            ref = self.at(axis, self.pos(axis, 0), span)
            ref[...] = (ref[...].astype(F32) + self.main[h, 0].astype(F32) + self.main[h, 1].astype(F32)).astype(BF16)
            for s, way in enumerate(self.ways(cross)):
                d = (0, 2) if cross == "y" else (2, 0)
                self.link.start(7 + 2 * h + s, self.one(d[0], d[1], self.cols[axis][s]),
                                self.relay2.at[h, s], p.dev(way))

    def far2_add(self):
        p = self.place
        for h, (axis, cross) in enumerate((("x", "y"), ("y", "x"))):
            for s, way in enumerate(self.ways(cross)):
                self.link.wait(7 + 2 * h + s, self.relay2.at[h, s])
                ref = self.one(way[0], way[1], self.cols[axis][s])
                ref[...] = (ref[...].astype(F32) + self.relay2[h, s].astype(F32)).astype(BF16)
                self.link.start(11 + h, self.one(way[0], way[1], self.cols[axis][2]),
                                self.main2.at[h, s], p.dev(way))

    def finish(self, out_ref, inv):
        for h in range(2):
            self.link.wait(11 + h, self.main2.at[h])
            out_ref[:, pl.ds(2 * self.q * h, 2 * self.q)] = (
                self.acc[h] + self.main2[h, 0].astype(F32) + self.main2[h, 1].astype(F32)) * inv


class Spread:
    def __init__(self, link, send_sems, mine, stage, relay, mid, final):
        self.link, self.place, self.sems = link, link.place, send_sems
        self.mine, self.stage, self.relay, self.mid, self.final = mine, stage, relay, mid, final

    def pair_send(self):
        p = self.place
        self.link.start(0, self.mine.at[1 - p.core], self.stage.at[p.core], p.dev((0, 0), True), self.sems[0])

    def pair_take(self):
        p = self.place
        self.stage[p.core] = self.mine[p.core]
        self.link.wait(0, self.stage.at[1 - p.core])

    def src(self, h, pos, lo, hi):
        rest = pl.ds(lo, hi - lo)
        return self.stage.at[h, rest, pos] if h == 0 else self.stage.at[h, pos, rest]

    def first_send(self):
        p = self.place
        s2 = p.side // 2
        for h in range(2):
            here = p.x if h == 0 else p.y
            ways = (XP, XM) if h == 0 else (YP, YM)
            pos = p.col if h == 0 else p.row
            for s, way in enumerate(ways):
                self.link.start(1 + 2 * h + s, self.src(h, pos(2), s * s2, s * s2 + s2), self.relay.at[h, s], p.dev(way), self.sems[1])
            for s, way in enumerate(ways):
                d = 1 if s == 0 else -1
                self.link.start(5 + h, self.src(h, pos(d), 0, p.side), self.mid.at[h, here], p.dev(way), self.sems[1])
            self.mid[h, here] = self.src(h, here, 0, p.side)[...]

    def first_relay(self):
        p = self.place
        s2 = p.side // 2
        for h in range(2):
            ways = (XP, XM) if h == 0 else (YP, YM)
            pos = p.col if h == 0 else p.row
            for s, way in enumerate(ways):
                self.link.wait(1 + 2 * h + s, self.relay.at[h, s])
                self.link.start(5 + h, self.relay.at[h, s],
                                self.mid.at[h, pos(-1 if s == 0 else 1), pl.ds(s * s2, s2)], p.dev(way), self.sems[1])

    def second_send(self):
        p = self.place
        s2 = p.side // 2
        for h in range(2):
            self.link.wait(5 + h, self.mid.at[h, 0:p.side - 1])
            cross = p.row if h == 0 else p.col
            ways = (YP, YM) if h == 0 else (XP, XM)
            for s, way in enumerate(ways):
                self.link.start(7 + 2 * h + s, self.mid.at[h, pl.ds(s * s2, s2), cross(2)],
                                self.relay.at[2 + h, s], p.dev(way), self.sems[2])
            for s, way in enumerate(ways):
                self.link.start(11, self.mid.at[h, :, cross(1 if s == 0 else -1)],
                                self.dst(h, cross(0), 0, p.side), p.dev(way), self.sems[2])
            self.dst(h, cross(0), 0, p.side)[...] = self.mid[h, :, cross(0)]

    def dst(self, h, pos, lo, hi):
        rest = pl.ds(lo, hi - lo)
        return self.final.at[pos, rest, h] if h == 0 else self.final.at[rest, pos, h]

    def second_relay(self):
        p = self.place
        s2 = p.side // 2
        for h in range(2):
            cross = p.row if h == 0 else p.col
            ways = (YP, YM) if h == 0 else (XP, XM)
            for s, way in enumerate(ways):
                self.link.wait(7 + 2 * h + s, self.relay.at[2 + h, s])
                self.link.start(11, self.relay.at[2 + h, s],
                                self.dst(h, cross(-1 if s == 0 else 1), s * s2, s * s2 + s2), p.dev(way), self.sems[2])

    def finish(self):
        self.link.wait(11, self.mid.at[:, 0:self.place.side - 1])

    def drain(self):
        self.link.drain(self.mine.at[0], self.sems[0])
        self.link.drain(self.mid, self.sems[1])
        self.link.drain(self.mid, self.sems[2])


class Total:
    def __init__(self, link, sent, got):
        self.link, self.place, self.sent, self.got = link, link.place, sent, got
        p = self.place
        odd = lambda c: c + 1 - 2 * lax.rem(c, 2)
        self.targets = [p.dev((0, 0), True), p.at(odd(p.x), p.y), p.at(p.side - 1 - p.x, p.y), p.at(p.x, odd(p.y)), p.at(p.x, p.side - 1 - p.y)]

    def send(self, i):
        self.link.start(i, self.sent.at[i], self.got.at[i], self.targets[i])

    def first(self, value):
        self.sent[0] = jnp.broadcast_to(value, self.sent.shape[1:])
        self.send(0)

    def step(self, i):
        self.link.wait(i, self.got.at[i])
        value = self.sent[i] + self.got[i]
        if i + 1 < len(self.targets):
            self.sent[i + 1] = value
            self.send(i + 1)
        return value

    def drain(self):
        self.link.drain(self.sent)


def split3(value):
    hi = value.astype(BF16)
    rest = value - hi.astype(F32)
    mid = rest.astype(BF16)
    lo = (rest - mid.astype(F32)).astype(BF16)
    return hi, mid, lo


def kernel(n, acts_hbm, wcat, tmine,
           loss_ref, dx_ref, g0_ref, g1_ref, g2_ref, un0_ref, un1_ref, un2_ref, v0_ref, v1_ref, v2_ref, sig_ref,
           wa, wb, x0, x1, x2, xt0, xt1, xt2, yt0, yt1, yt2, mt, mask0, mask1, lowt, low, low2, dxa, dxb, uc, sq, vbuf,
           tstage, trelay, tmid, tfinal, losssent, lossgot,
           d0, d1, d2, m0, m1, m2,
           ra0, rb0, rc0, re0, rf0, ra1, rb1, rc1, re1, rf1, ra2, rb2, rc2, re2, rf2,
           acts_sem, send_sems, w_recv, dx_recv, rs_recv, t_recv, l_recv):
    p = Place(n)
    side = p.side
    rows = x0.shape[0]
    wr = wcat.shape[0]
    total_rows, k0 = dx_ref.shape
    k1 = wb.shape[1]
    wide = k0 + LANES
    width = wa.shape[0]
    mine = pl.ds(pl.multiple_of(p.me * wr, wr), wr)
    w0 = wa.at[:, pl.ds(0, k0)]
    ucols = wa.at[:, pl.ds(k0, LANES)]
    w1 = wa.at[:, pl.ds(wide, k1)]
    w2 = wb

    acts_load = pltpu.make_async_copy(acts_hbm.at[pl.ds(pl.multiple_of(p.me * rows, rows), rows)], x0, acts_sem)
    acts_load.start()

    barrier = pltpu.get_barrier_semaphore()
    peers = [p.dev(way) for way in (XP, XM, YP, YM)] + [p.dev((0, 0), True)]
    for peer in peers:
        pl.semaphore_signal(barrier, inc=1, device_id={"model": peer}, device_id_type=MESH)
    pl.semaphore_wait(barrier, len(peers))

    def gather_weight(i, ref):
        def ref_at(dev, s):
            return ref.at[pl.ds(pl.multiple_of(dev * wr, wr), wr), pl.ds(s[0], s[1] - s[0])]

        tiles = ref.shape[1] // LANES
        cuts = [LANES * ((tiles * k) // 4) for k in range(5)]
        return Gather(Link(p, send_sems.at[i], w_recv.at[i]), ref_at, lambda k: ref.at[pl.ds(0, k * wr)], cuts)

    ga, gb = gather_weight(0, wa), gather_weight(1, wb)
    for g, ref, lo in ((ga, wa, 0), (gb, wb, wa.shape[1])):
        own = wcat.at[:, pl.ds(lo, ref.shape[1])]
        g.step0(own)
        ref[mine] = own[...]

    spread = Spread(Link(p, send_sems.at[2], t_recv), [send_sems.at[k] for k in (2, 3, 4)], tmine, tstage, trelay, tmid, tfinal)
    spread.pair_send()
    eye_big = (lax.broadcasted_iota(jnp.int32, (TILE, TILE), 0) == lax.broadcasted_iota(jnp.int32, (TILE, TILE), 1)).astype(BF16)
    eye_small = eye_big[0:SUB, 0:SUB]

    def turn(src, dst):
        for j in range(max(src.shape) // TILE):
            at = pl.ds(j * TILE, TILE)
            if src.shape[0] > TILE:
                dst[:, at] = dot(eye_big, src[at, :], NT).astype(BF16)
            else:
                dst[at, :] = dot(eye_big, src[:, at], NT).astype(BF16)

    def power(i, w_ref):
        picked = (lax.broadcasted_iota(jnp.int32, (SUB, LANES), 1) == i).astype(BF16)
        u_row = dot(picked, ucols[...], NT).astype(BF16)
        for step in range(POWER_STEPS):
            pv = dot(u_row, w_ref[...], NN)
            norm = jnp.sqrt(jnp.sum(pv * pv, axis=1, keepdims=True))
            v16 = (pv / jnp.maximum(norm, NORM_FLOOR)).astype(BF16)
            sv = dot(w_ref[...], v16, NT)
            sigma = jnp.sqrt(jnp.sum(sv * sv, axis=0, keepdims=True))
            ucol = sv / sigma
            if step + 1 < POWER_STEPS:
                u_row = dot(eye_small, ucol.astype(BF16), NT).astype(BF16)
        uc[i] = ucol
        vbuf[i, :, pl.ds(0, v16.shape[1])] = v16
        sigma = sigma[0:1, 0:1]
        own = dot(v16, w_ref[mine, :], NT) / sigma
        (un0_ref, un1_ref, un2_ref)[i][...] = own[0:1]
        (v0_ref, v1_ref, v2_ref)[i][...] = v16[0:1]
        return sigma

    def forward(w_ref, xt_ref, inv, y_ref, next_ref, mask_ref):
        for j in range(width // FTILE):
            at = pl.ds(j * FTILE, FTILE)
            y = dot(w_ref[at, :], xt_ref[...], NN) * inv
            y_ref[at, :] = y
            if next_ref is not None:
                next_ref[at, :] = jnp.where(y >= 0, y, LEAK * y).astype(BF16)
                mask_ref[at, :] = jnp.where(y >= 0, 1.0, 0.0).astype(BF16)

    acts_load.wait()
    turn(x0, xt0)
    ga.step1()
    gb.step1()
    spread.pair_take()
    ga.step2()
    gb.step2()
    spread.first_send()
    ga.step3()
    gb.step3()
    ga.step4()
    spread.first_relay()
    ga.finish()
    sa = power(0, w0)
    inva = 1.0 / sa
    spread.second_send()
    gb.step4()
    forward(w0, xt0, inva, yt0, xt1, mt)
    turn(xt1, x1)
    turn(mt, mask0)
    sb = power(1, w1)
    spread.second_relay()
    invb = 1.0 / sb
    forward(w1, xt1, invb, yt1, xt2, mt)
    gb.finish()
    sc = power(2, w2)
    invc = 1.0 / sc
    forward(w2, xt2, invc, yt2, None, None)
    turn(xt2, x2)
    turn(mt, mask1)
    spread.finish()

    lane1 = lax.broadcasted_iota(jnp.int32, (1, LANES), 1)
    sig_ref[...] = jnp.where(lane1 == 0, sa, jnp.where(lane1 == 1, sb, sc))

    scale = 1.0 / total_rows
    zero_row = jnp.zeros((1, rows), F32)

    def down(value):
        return jnp.sum(value, axis=0, keepdims=True)

    loss = zero_row
    corr = zero_row
    for j in range(side):
        at = pl.ds(j * TILE, TILE)
        y = yt2[at, :]
        residual = y - tfinal[j].reshape(TILE, rows).astype(F32)
        g = residual * scale
        lowt[at, :] = g.astype(BF16)
        loss = loss + down(residual * residual)
        corr = corr + down(g * y)
    whole = Total(Link(p, send_sems.at[10], l_recv), losssent, lossgot)
    whole.first(jnp.sum(loss, axis=1, keepdims=True))

    def share(i, x_ref, d_ref, corr):
        corr = jnp.sum(corr, axis=1, keepdims=True)
        parts = split3(uc[i] * (-corr))
        lane = lax.broadcasted_iota(jnp.int32, (width, SUB), 1)
        uu = jnp.zeros((width, SUB), F32)
        for k, part in enumerate(parts):
            uu = jnp.where(lane == k, part.astype(F32), uu)
        sq[...] = uu.astype(BF16)

        def body(j, carry):
            at = pl.ds(pl.multiple_of(j * TILE, TILE), TILE)
            full = dot(lowt[...], x_ref[:, at], NN) + dot(sq[...], vbuf[i, :, at], NN)
            d_ref[:, :, :, :, at] = full.astype(BF16).reshape(side, side, CORES, wr, TILE)
            return carry

        lax.fori_loop(0, x_ref.shape[1] // TILE, body, 0)

    def back(w_ref, inv, low_ref, out_ref, mask_ref, next_ref):
        for j in range(w_ref.shape[1] // TILE):
            at = pl.ds(j * TILE, TILE)
            dx = (dot(low_ref[...], w_ref[:, at], NN) * inv).astype(BF16)
            out_ref[:, at] = dx
            if mask_ref is not None:
                next_ref[:, at] = jnp.where(mask_ref[:, at].astype(F32) > 0.5, dx.astype(F32), LEAK * dx.astype(F32)).astype(BF16)

    def columns(dx_ref, yt_ref):
        corr = zero_row
        for j in range(width // TILE):
            at = pl.ds(j * TILE, TILE)
            y = yt_ref[at, :]
            g = dot(eye_big, dx_ref[:, at], NT) * jnp.where(y >= 0, 1.0, LEAK)
            lowt[at, :] = g.astype(BF16)
            corr = corr + down(g * y)
        return corr

    def reducer(i, blocks, mate, relay, main, relay2, main2, acc, cols):
        return Reduce(Link(p, send_sems.at[5 + i], rs_recv.at[i]), blocks, mate, relay, main, relay2, main2, acc, cols)

    rc = reducer(2, d2, m2, ra2, rb2, rc2, re2, rf2, k1)
    rb = reducer(1, d1, m1, ra1, rb1, rc1, re1, rf1, k1)
    ra = reducer(0, d0, m0, ra0, rb0, rc0, re0, rf0, k0)
    out_rows = pl.ds(pl.multiple_of(p.me * rows, rows), rows)
    turn(lowt, low)
    back(w2, invc, low, dxa, mask1, low2)
    back(w1, invb, low2, dxb, mask0, low)
    back(w0, inva, low, dx_ref.at[out_rows], None, None)

    part = rows // DX_PARTS
    gd = []
    for i in range(DX_PARTS):
        def dx_at(dev, s, i=i):
            return dx_ref.at[pl.ds(pl.multiple_of(dev * rows + (i * part + s[0]), SUB), s[1] - s[0])]

        gd.append(Gather(Link(p, send_sems.at[8 + i], dx_recv.at[i]), dx_at, lambda k: dx_ref.at[pl.ds(0, k * part)], [part * k // 4 for k in range(5)]))
    for g in gd:
        g.step0()
    share(2, x2, d2, corr)
    rc.pair_send()
    corr = columns(dxa, yt1)
    share(1, x1, d1, corr)
    rb.pair_send()
    rc.pair_add()
    rc.far_send()
    whole.step(0)
    corr = columns(dxb, yt0)
    share(0, x0, d0, corr)
    ra.pair_send()
    rb.pair_add()
    rb.far_send()
    gd[0].step1()
    ra.pair_add()
    ra.far_send()
    whole.step(1)
    rc.far_add()
    gd[1].step1()
    rb.far_add()
    ra.far_add()
    whole.step(2)
    rc.near_add()
    rb.near_add()
    ra.near_add()
    whole.step(3)
    gd[0].step2()
    rc.far2_add()
    rb.far2_add()
    ra.far2_add()
    loss_ref[...] = whole.step(4)[0:1, 0:1] * (0.5 * scale)
    gd[1].step2()
    rc.finish(g2_ref, invc)
    rb.finish(g1_ref, invb)
    ra.finish(g0_ref, inva)
    gd[0].step3()
    gd[1].step3()
    gd[0].step4()
    gd[1].step4()
    for g in gd:
        g.finish()
    ga.drain()
    gb.drain()
    spread.drain()
    whole.drain()
    ra.link.drain(dx_ref.at[pl.ds(0, (n - 1) * wr)])
    rb.link.drain(wb.at[pl.ds(0, (n - 1) * wr)])
    rc.link.drain(wb.at[pl.ds(0, (n - 1) * wr)])
    for g in gd:
        g.drain()


def device_program(n, acts_in, w_first, w_middle, w_last, u_first, u_middle, u_last, target):
    side = math.isqrt(n // CORES)
    total_rows, k0 = acts_in.shape
    rows = total_rows // n
    wr, k1 = w_middle.shape
    width = wr * n
    tcols = target.shape[1]
    hbm = pl.BlockSpec(memory_space=pltpu.HBM)
    chips = side * side

    def reduce_bufs(k):
        q = k // 4
        return [pltpu.VMEM((2, 2, side, wr, q), BF16), pltpu.VMEM((2, 2, side, wr, 2 * q), BF16),
                pltpu.VMEM((2, 2, wr, q), BF16), pltpu.VMEM((2, 2, wr, 2 * q), BF16), pltpu.VMEM((2, wr, 2 * q), F32)]

    vmem = pl.BlockSpec(memory_space=pltpu.VMEM)
    out_shape = (
        jax.ShapeDtypeStruct((1, 1), F32), jax.ShapeDtypeStruct((total_rows, k0), BF16),
        jax.ShapeDtypeStruct((wr, k0), F32), jax.ShapeDtypeStruct((wr, k1), F32), jax.ShapeDtypeStruct((wr, k1), F32),
        jax.ShapeDtypeStruct((1, wr), F32), jax.ShapeDtypeStruct((1, wr), F32), jax.ShapeDtypeStruct((1, wr), F32),
        jax.ShapeDtypeStruct((1, k0), BF16), jax.ShapeDtypeStruct((1, k1), BF16), jax.ShapeDtypeStruct((1, k1), BF16),
        jax.ShapeDtypeStruct((1, LANES), F32))
    scratch = [
        pltpu.VMEM((width, k0 + LANES + k1), BF16), pltpu.VMEM((width, k1), BF16),
        pltpu.VMEM((rows, k0), BF16), pltpu.VMEM((rows, k1), BF16), pltpu.VMEM((rows, k1), BF16),
        pltpu.VMEM((k0, rows), BF16), pltpu.VMEM((k1, rows), BF16), pltpu.VMEM((k1, rows), BF16),
        pltpu.VMEM((width, rows), F32), pltpu.VMEM((width, rows), F32), pltpu.VMEM((width, rows), F32),
        pltpu.VMEM((width, rows), BF16), pltpu.VMEM((rows, width), BF16), pltpu.VMEM((rows, width), BF16),
        pltpu.VMEM((width, rows), BF16), pltpu.VMEM((rows, width), BF16), pltpu.VMEM((rows, width), BF16),
        pltpu.VMEM((rows, width), BF16), pltpu.VMEM((rows, width), BF16),
        pltpu.VMEM((3, width, SUB), F32), pltpu.VMEM((width, SUB), BF16), pltpu.VMEM((3, SUB, k1), BF16),
        pltpu.VMEM((CORES, side, side, tcols, rows), BF16),
        pltpu.VMEM((4, 2, side // 2, tcols, rows), BF16), pltpu.VMEM((2, side, side, tcols, rows), BF16),
        pltpu.VMEM((side, side, CORES, tcols, rows), BF16),
        pltpu.VMEM((5, 8, LANES), F32), pltpu.VMEM((5, 8, LANES), F32),
        pltpu.VMEM((side, side, CORES, wr, k0), BF16), pltpu.VMEM((side, side, CORES, wr, k1), BF16), pltpu.VMEM((side, side, CORES, wr, k1), BF16),
        pltpu.VMEM((side, side, wr, k0), BF16), pltpu.VMEM((side, side, wr, k1), BF16), pltpu.VMEM((side, side, wr, k1), BF16),
        *reduce_bufs(k0), *reduce_bufs(k1), *reduce_bufs(k1),
        pltpu.SemaphoreType.DMA, pltpu.SemaphoreType.DMA((11,)),
        pltpu.SemaphoreType.DMA((2, chips)), pltpu.SemaphoreType.DMA((DX_PARTS, chips)),
        pltpu.SemaphoreType.DMA((3, 13)), pltpu.SemaphoreType.DMA((12,)), pltpu.SemaphoreType.DMA((5,)),
    ]
    wcat, tmine = pl.pallas_call(
        take,
        out_shape=(jax.ShapeDtypeStruct((wr, k0 + LANES + 2 * k1), BF16),
                   jax.ShapeDtypeStruct((CORES, side, side, tcols, rows), BF16)),
        in_specs=[hbm] * 7,
        out_specs=(vmem, vmem),
        scratch_shapes=[pltpu.VMEM((3, 1, wr), F32), pltpu.SemaphoreType.DMA((7,))],
        compiler_params=pltpu.CompilerParams(vmem_limit_bytes=TAKE_LIMIT),
        name="take",
    )(w_first, w_middle, w_last, u_first.reshape(1, wr), u_middle.reshape(1, wr), u_last.reshape(1, wr), target.T)
    outs = pl.pallas_call(
        functools.partial(kernel, n),
        out_shape=out_shape,
        in_specs=[hbm, vmem, vmem],
        out_specs=(vmem,) * len(out_shape),
        scratch_shapes=scratch,
        compiler_params=pltpu.CompilerParams(collective_id=0, has_side_effects=True, vmem_limit_bytes=VMEM_LIMIT),
        name="stack",
    )(acts_in, wcat, tmine)
    final = tuple(jax.ShapeDtypeStruct(shape, dtype) for shape, dtype in (
        ((1,), F32), ((total_rows, k0), BF16), ((wr, k0), F32), ((wr, k1), F32), ((wr, k1), F32),
        ((wr,), F32), ((wr,), F32), ((wr,), F32), ((k0,), BF16), ((k1,), BF16), ((k1,), BF16), ((3,), F32)))
    return pl.pallas_call(
        emit,
        out_shape=final,
        in_specs=[vmem] * len(final),
        out_specs=tuple(hbm if 1 <= i <= 4 else vmem for i in range(len(final))),
        scratch_shapes=[pltpu.SemaphoreType.DMA((4,))],
        compiler_params=pltpu.CompilerParams(vmem_limit_bytes=EMIT_LIMIT),
        name="emit",
    )(*outs)


def take(w0_hbm, w1_hbm, w2_hbm, u0_hbm, u1_hbm, u2_hbm, target_hbm, wcat, tmine, ubuf, sems):
    wr, k0 = w0_hbm.shape
    k1 = w1_hbm.shape[1]
    cores, side = tmine.shape[:2]
    rows = tmine.shape[-1]
    wide = k0 + LANES
    loads = [pltpu.make_async_copy(ref, ubuf.at[i], sems.at[i]) for i, ref in enumerate((u0_hbm, u1_hbm, u2_hbm))]
    for i, (ref, lo) in enumerate(((w0_hbm, 0), (w1_hbm, wide), (w2_hbm, wide + k1))):
        loads.append(pltpu.make_async_copy(ref, wcat.at[:, pl.ds(lo, ref.shape[1])], sems.at[3 + i]))
    for load in loads:
        load.start()

    def turn(j, carry):
        chip = j // cores
        part = tmine.at[lax.rem(j, cores), chip // side, lax.rem(chip, side)]
        pltpu.make_async_copy(target_hbm.at[:, pl.ds(pl.multiple_of(j * rows, rows), rows)], part, sems.at[6]).start()
        return carry

    lax.fori_loop(0, cores * side * side, turn, 0)
    lane = lax.broadcasted_iota(jnp.int32, (wr, LANES), 1)
    eye = (lax.broadcasted_iota(jnp.int32, (wr, wr), 0) == lax.broadcasted_iota(jnp.int32, (wr, wr), 1))
    uext = jnp.zeros((wr, LANES), F32)
    for i in range(3):
        loads[i].wait()
        column = jnp.sum(jnp.where(eye, jnp.broadcast_to(ubuf[i], (wr, wr)), 0.0), axis=1, keepdims=True)
        uext = jnp.where(lane == i, column, uext)
    wcat[:, pl.ds(k0, LANES)] = uext.astype(BF16)
    for load in loads[3:]:
        load.wait()
    pltpu.make_async_copy(tmine, tmine, sems.at[6]).wait()


def emit(*refs):
    count = (len(refs) - 1) // 2
    ins, outs, sems = refs[:count], refs[count:2 * count], refs[-1]
    copies = [pltpu.make_async_copy(ins[i], outs[i], sems.at[i - 1]) for i in range(1, 5)]
    for copy in copies:
        copy.start()
    for i in (0, *range(5, count)):
        outs[i][...] = ins[i][0, 0:outs[i].shape[0]]
    for copy in copies:
        copy.wait()


def solution(mesh):
    n = mesh.shape["model"]
    row_spec = P("rep", None)
    weight_spec = P(("rep", "model"), None)
    vector_spec = P(("rep", "model"))
    group_spec = P("rep")
    in_specs = (row_spec, weight_spec, weight_spec, weight_spec, vector_spec, vector_spec, vector_spec, P("rep", "model"))
    out_specs = (group_spec, row_spec, weight_spec, weight_spec, weight_spec, vector_spec, vector_spec, vector_spec, group_spec, group_spec, group_spec, group_spec)
    return jax.shard_map(lambda *args: device_program(n, *args), mesh=mesh, in_specs=in_specs, out_specs=out_specs, check_vma=False)
```

```python
import functools
import math

import jax
import jax.numpy as jnp
from jax import lax
from jax.experimental import pallas as pl
from jax.experimental.pallas import tpu as pltpu
from jax.sharding import PartitionSpec as P

LEAK = 0.2
NORM_FLOOR = 1e-12
POWER_STEPS = 2
MESH = pl.DeviceIdType.MESH
F32 = jnp.float32
BF16 = jnp.bfloat16
NN = (((1,), (0,)), ((), ()))
NT = (((1,), (1,)), ((), ()))
TN = (((0,), (0,)), ((), ()))
CORES = 2
LANES = 128
SUB = 16
TILE = 256
FTILE = 256
VMEM_LIMIT = 40 * 1024 * 1024
EMIT_PARTS = 16
EMIT_LIMIT = 12 * 1024 * 1024
DX_PARTS = 2
XP, XM, YP, YM = (1, 0), (-1, 0), (0, 1), (0, -1)


def dot(lhs, rhs, dims):
    return lax.dot_general(lhs, rhs, dims, preferred_element_type=F32)


class Place:
    def __init__(self, n):
        self.side = math.isqrt(n // CORES)
        me = lax.axis_index("model")
        self.me = me
        self.core = lax.rem(me, CORES)
        self.x = lax.rem(me // CORES, self.side)
        self.y = me // (CORES * self.side)

    def col(self, dx):
        return lax.rem(self.x + (dx + self.side), self.side)

    def row(self, dy):
        return lax.rem(self.y + (dy + self.side), self.side)

    def dev(self, rel, other=False):
        core = 1 - self.core if other else self.core
        return (self.row(rel[1]) * self.side + self.col(rel[0])) * CORES + core

    def at(self, x, y):
        return (y * self.side + x) * CORES + self.core

    def norm(self, rel):
        s = self.side
        half = s // 2
        return tuple((r + half - 1) % s - (half - 1) for r in rel)


class Link:
    def __init__(self, place, send_sem, recv_sems):
        self.place, self.send_sem, self.recv_sems = place, send_sem, recv_sems

    def copy(self, i, src, dst, target, send_sem=None):
        return pltpu.make_async_remote_copy(
            src_ref=src, dst_ref=dst, send_sem=self.send_sem if send_sem is None else send_sem,
            recv_sem=self.recv_sems.at[i], device_id={"model": target}, device_id_type=MESH)

    def start(self, i, src, dst, target, send_sem=None):
        self.copy(i, src, dst, target, send_sem).start()

    def wait(self, i, dst):
        self.copy(i, dst, dst, self.place.dev((0, 0), True)).wait_recv()

    def drain(self, sent, send_sem=None):
        self.copy(0, sent, sent, self.place.dev((0, 0), True), send_sem).wait_send()


class Gather:
    def __init__(self, link, ref_at, bulk, cuts):
        self.link, self.ref_at, self.bulk, self.place = link, ref_at, bulk, link.place
        a, b, c, d, e = cuts
        self.full, self.mid, self.outer = ((a, e),), ((b, d),), ((a, b), (d, e))
        self.half = {"x": ((a, c),), "y": ((c, e),)}
        self.fwd = {"x": ((b, c),), "y": ((c, d),)}
        self.bwd = {"x": ((a, b),), "y": ((d, e),)}

    def number(self, rel):
        return (rel[1] + 1) * self.place.side + rel[0] + 1

    def start(self, rel, spans, way, src=None):
        there = self.number(self.place.norm((rel[0] - way[0], rel[1] - way[1])))
        for s in spans:
            ref = self.ref_at(self.place.dev(rel), s)
            self.link.start(there, ref if src is None else src, ref, self.place.dev(way))

    def take(self, rel):
        self.link.wait(self.number(rel), self.ref_at(self.place.dev(rel), self.full[0]))

    def mate(self, rel, src=None):
        ref = self.ref_at(self.place.dev(rel), self.full[0])
        self.link.start(self.number((0, 0)), ref if src is None else src, ref, self.place.dev((0, 0), True))

    def cross(self, rel, axis):
        for way in ((YP, YM) if axis == "x" else (XP, XM)):
            self.start(rel, self.half[axis], way)

    def relay(self, rel, axis, first):
        off = rel[0] if axis == "x" else rel[1]
        way = {("x", -1): XP, ("x", 1): XM, ("y", -1): YP, ("y", 1): YM}[(axis, off)]
        self.start(rel, (self.fwd if off < 0 else self.bwd)[first], way)

    def step0(self, src=None):
        for way in (XP, YP, XM, YM):
            self.start((0, 0), self.full, way, src)
        self.mate((0, 0), src)

    def step1(self):
        for way in (XP, YP, XM, YM):
            rel = (-way[0], -way[1])
            self.take(rel)
            self.start(rel, self.mid if way in (XP, YP) else self.outer, way)
            self.cross(rel, "x" if way[0] else "y")
            self.mate(rel)

    def step2(self):
        for rel, axis in (((2, 0), "x"), ((0, 2), "y")):
            self.take(rel)
            self.cross(rel, axis)
            self.mate(rel)
        for rel in ((-1, -1), (-1, 1), (1, -1), (1, 1)):
            self.take(rel)
            self.relay(rel, "y", "x")
            self.relay(rel, "x", "y")
            self.mate(rel)

    def step3(self):
        for d in (-1, 1):
            self.take((2, d))
            self.relay((2, d), "y", "x")
            self.mate((2, d))
            self.take((d, 2))
            self.relay((d, 2), "x", "y")
            self.mate((d, 2))

    def step4(self):
        self.take((2, 2))
        self.mate((2, 2))

    def finish(self):
        self.link.wait(self.number((0, 0)), self.bulk(self.place.side ** 2))

    def drain(self):
        self.link.drain(self.bulk(CORES * self.place.side ** 2 - 1))


class Reduce:
    def __init__(self, link, blocks, mate, relay, main, relay2, main2, acc, width):
        self.link, self.place = link, link.place
        self.blocks, self.mate = blocks, mate
        self.relay, self.main, self.relay2, self.main2, self.acc = relay, main, relay2, main2, acc
        q = width // 4
        self.q = q
        self.cols = {"x": ((q, 2 * q), (0, q), (0, 2 * q)), "y": ((2 * q, 3 * q), (3 * q, 4 * q), (2 * q, 4 * q))}

    def at(self, axis, pos, span):
        cols = pl.ds(span[0], span[1] - span[0])
        if axis == "x":
            return self.blocks.at[:, pos, self.place.core, :, cols]
        return self.blocks.at[pos, :, self.place.core, :, cols]

    def one(self, dx, dy, span):
        return self.blocks.at[self.place.row(dy), self.place.col(dx), self.place.core, :, pl.ds(span[0], span[1] - span[0])]

    def pair_send(self):
        p = self.place
        self.link.start(0, self.blocks.at[:, :, 1 - p.core], self.mate, p.dev((0, 0), True))

    def pair_add(self):
        p = self.place
        self.link.wait(0, self.mate)
        for k in range(p.side):
            mine = self.blocks.at[k, :, p.core]
            mine[...] = (mine[...].astype(F32) + self.mate[k].astype(F32)).astype(BF16)

    def pos(self, axis, d):
        return self.place.col(d) if axis == "x" else self.place.row(d)

    def ways(self, axis):
        return (XP, XM) if axis == "x" else (YP, YM)

    def far_send(self):
        for h, axis in enumerate(("x", "y")):
            for s, way in enumerate(self.ways(axis)):
                self.link.start(1 + 2 * h + s, self.at(axis, self.pos(axis, 2), self.cols[axis][s]),
                                self.relay.at[h, s], self.place.dev(way))

    def far_add(self):
        for h, axis in enumerate(("x", "y")):
            for s, way in enumerate(self.ways(axis)):
                self.link.wait(1 + 2 * h + s, self.relay.at[h, s])
                step = 1 if s == 0 else -1
                ref = self.at(axis, self.pos(axis, step), self.cols[axis][s])
                ref[...] = (ref[...].astype(F32) + self.relay[h, s].astype(F32)).astype(BF16)
                self.link.start(5 + h, self.at(axis, self.pos(axis, step), self.cols[axis][2]),
                                self.main.at[h, s], self.place.dev(way))

    def near_add(self):
        p = self.place
        for h, (axis, cross) in enumerate((("x", "y"), ("y", "x"))):
            self.link.wait(5 + h, self.main.at[h])
            own = self.pos(cross, 0)
            span = self.cols[axis][2]
            self.acc[h] = (self.one(0, 0, span)[...].astype(F32) + self.main[h, 0, own].astype(F32)
                           + self.main[h, 1, own].astype(F32))
            ref = self.at(axis, self.pos(axis, 0), span)
            ref[...] = (ref[...].astype(F32) + self.main[h, 0].astype(F32) + self.main[h, 1].astype(F32)).astype(BF16)
            for s, way in enumerate(self.ways(cross)):
                d = (0, 2) if cross == "y" else (2, 0)
                self.link.start(7 + 2 * h + s, self.one(d[0], d[1], self.cols[axis][s]),
                                self.relay2.at[h, s], p.dev(way))

    def far2_add(self):
        p = self.place
        for h, (axis, cross) in enumerate((("x", "y"), ("y", "x"))):
            for s, way in enumerate(self.ways(cross)):
                self.link.wait(7 + 2 * h + s, self.relay2.at[h, s])
                ref = self.one(way[0], way[1], self.cols[axis][s])
                ref[...] = (ref[...].astype(F32) + self.relay2[h, s].astype(F32)).astype(BF16)
                self.link.start(11 + h, self.one(way[0], way[1], self.cols[axis][2]),
                                self.main2.at[h, s], p.dev(way))

    def finish(self, out_ref, inv):
        for h in range(2):
            self.link.wait(11 + h, self.main2.at[h])
            out_ref[:, pl.ds(2 * self.q * h, 2 * self.q)] = (
                self.acc[h] + self.main2[h, 0].astype(F32) + self.main2[h, 1].astype(F32)) * inv


class Spread:
    def __init__(self, link, send_sems, mine, stage, relay, mid, final):
        self.link, self.place, self.sems = link, link.place, send_sems
        self.mine, self.stage, self.relay, self.mid, self.final = mine, stage, relay, mid, final

    def pair_send(self):
        p = self.place
        self.link.start(0, self.mine.at[1 - p.core], self.stage.at[p.core], p.dev((0, 0), True), self.sems[0])

    def pair_take(self):
        p = self.place
        self.stage[p.core] = self.mine[p.core]
        self.link.wait(0, self.stage.at[1 - p.core])

    def src(self, h, pos, lo, hi):
        rest = pl.ds(lo, hi - lo)
        return self.stage.at[h, rest, pos] if h == 0 else self.stage.at[h, pos, rest]

    def first_send(self):
        p = self.place
        s2 = p.side // 2
        for h in range(2):
            here = p.x if h == 0 else p.y
            ways = (XP, XM) if h == 0 else (YP, YM)
            pos = p.col if h == 0 else p.row
            for s, way in enumerate(ways):
                self.link.start(1 + 2 * h + s, self.src(h, pos(2), s * s2, s * s2 + s2), self.relay.at[h, s], p.dev(way), self.sems[1])
            for s, way in enumerate(ways):
                d = 1 if s == 0 else -1
                self.link.start(5 + h, self.src(h, pos(d), 0, p.side), self.mid.at[h, here], p.dev(way), self.sems[1])
            self.mid[h, here] = self.src(h, here, 0, p.side)[...]

    def first_relay(self):
        p = self.place
        s2 = p.side // 2
        for h in range(2):
            ways = (XP, XM) if h == 0 else (YP, YM)
            pos = p.col if h == 0 else p.row
            for s, way in enumerate(ways):
                self.link.wait(1 + 2 * h + s, self.relay.at[h, s])
                self.link.start(5 + h, self.relay.at[h, s],
                                self.mid.at[h, pos(-1 if s == 0 else 1), pl.ds(s * s2, s2)], p.dev(way), self.sems[1])

    def second_send(self):
        p = self.place
        s2 = p.side // 2
        for h in range(2):
            self.link.wait(5 + h, self.mid.at[h, 0:p.side - 1])
            cross = p.row if h == 0 else p.col
            ways = (YP, YM) if h == 0 else (XP, XM)
            for s, way in enumerate(ways):
                self.link.start(7 + 2 * h + s, self.mid.at[h, pl.ds(s * s2, s2), cross(2)],
                                self.relay.at[2 + h, s], p.dev(way), self.sems[2])
            for s, way in enumerate(ways):
                self.link.start(11, self.mid.at[h, :, cross(1 if s == 0 else -1)],
                                self.dst(h, cross(0), 0, p.side), p.dev(way), self.sems[2])
            self.dst(h, cross(0), 0, p.side)[...] = self.mid[h, :, cross(0)]

    def dst(self, h, pos, lo, hi):
        rest = pl.ds(lo, hi - lo)
        return self.final.at[pos, rest, h] if h == 0 else self.final.at[rest, pos, h]

    def second_relay(self):
        p = self.place
        s2 = p.side // 2
        for h in range(2):
            cross = p.row if h == 0 else p.col
            ways = (YP, YM) if h == 0 else (XP, XM)
            for s, way in enumerate(ways):
                self.link.wait(7 + 2 * h + s, self.relay.at[2 + h, s])
                self.link.start(11, self.relay.at[2 + h, s],
                                self.dst(h, cross(-1 if s == 0 else 1), s * s2, s * s2 + s2), p.dev(way), self.sems[2])

    def finish(self):
        self.link.wait(11, self.mid.at[:, 0:self.place.side - 1])

    def drain(self):
        self.link.drain(self.mine.at[0], self.sems[0])
        self.link.drain(self.mid, self.sems[1])
        self.link.drain(self.mid, self.sems[2])


class Total:
    def __init__(self, link, sent, got):
        self.link, self.place, self.sent, self.got = link, link.place, sent, got
        p = self.place
        odd = lambda c: c + 1 - 2 * lax.rem(c, 2)
        self.targets = [p.dev((0, 0), True), p.at(odd(p.x), p.y), p.at(p.side - 1 - p.x, p.y), p.at(p.x, odd(p.y)), p.at(p.x, p.side - 1 - p.y)]

    def send(self, i):
        self.link.start(i, self.sent.at[i], self.got.at[i], self.targets[i])

    def first(self, value):
        self.sent[0] = jnp.broadcast_to(value, self.sent.shape[1:])
        self.send(0)

    def step(self, i):
        self.link.wait(i, self.got.at[i])
        value = self.sent[i] + self.got[i]
        if i + 1 < len(self.targets):
            self.sent[i + 1] = value
            self.send(i + 1)
        return value

    def drain(self):
        self.link.drain(self.sent)


def split3(value):
    hi = value.astype(BF16)
    rest = value - hi.astype(F32)
    mid = rest.astype(BF16)
    lo = (rest - mid.astype(F32)).astype(BF16)
    return hi, mid, lo


def kernel(n, acts_hbm, w0_hbm, w1_hbm, w2_hbm, u0_hbm, u1_hbm, u2_hbm, target_hbm,
           loss_ref, dx_ref, g0_ref, g1_ref, g2_ref, un0_ref, un1_ref, un2_ref, v0_ref, v1_ref, v2_ref, sig_ref,
           wa, w1, w2, x0, x1, x2, xt0, xt1, xt2, yt0, yt1, yt2, mt, mask0, mask1, lowt, low, low2, dxa, dxb, uc, cu, vbuf, ustart,
           ubuf, tmine, tstage, trelay, tmid, tfinal, losssent, lossgot,
           d0, d1, d2, m0, m1, m2,
           ra0, rb0, rc0, re0, rf0, ra1, rb1, rc1, re1, rf1, ra2, rb2, rc2, re2, rf2,
           local_sems, send_sems, w_recv, dx_recv, rs_recv, t_recv, l_recv):
    p = Place(n)
    side = p.side
    rows = x0.shape[0]
    wr = w0_hbm.shape[0]
    total_rows, k0 = dx_ref.shape
    k1 = w1.shape[1]
    width = wa.shape[0]
    mine = pl.ds(pl.multiple_of(p.me * wr, wr), wr)
    w0 = wa.at[:, pl.ds(0, k0)]
    ucols = wa.at[:, pl.ds(k0, LANES)]

    loads = [
        pltpu.make_async_copy(u0_hbm, ubuf.at[0], local_sems.at[0]),
        pltpu.make_async_copy(u1_hbm, ubuf.at[1], local_sems.at[1]),
        pltpu.make_async_copy(u2_hbm, ubuf.at[2], local_sems.at[2]),
        pltpu.make_async_copy(w0_hbm, w0.at[mine], local_sems.at[3]),
        pltpu.make_async_copy(w1_hbm, w1.at[mine], local_sems.at[4]),
        pltpu.make_async_copy(w2_hbm, w2.at[mine], local_sems.at[5]),
    ]
    for load in loads:
        load.start()
    acts_load = pltpu.make_async_copy(acts_hbm.at[pl.ds(pl.multiple_of(p.me * rows, rows), rows)], x0, local_sems.at[6])
    acts_load.start()
    for j in range(n):
        part = tmine.at[j % CORES, j // (CORES * side), (j // CORES) % side]
        pltpu.make_async_copy(target_hbm.at[:, pl.ds(j * rows, rows)], part, local_sems.at[7]).start()

    barrier = pltpu.get_barrier_semaphore()
    peers = [p.dev(way) for way in (XP, XM, YP, YM)] + [p.dev((0, 0), True)]
    for peer in peers:
        pl.semaphore_signal(barrier, inc=1, device_id={"model": peer}, device_id_type=MESH)
    lane = lax.broadcasted_iota(jnp.int32, (wr, LANES), 1)
    eye = (lax.broadcasted_iota(jnp.int32, (wr, wr), 0) == lax.broadcasted_iota(jnp.int32, (wr, wr), 1))
    uext = jnp.zeros((wr, LANES), F32)
    for i in range(3):
        loads[i].wait()
        column = jnp.sum(jnp.where(eye, jnp.broadcast_to(ubuf[i], (wr, wr)), 0.0), axis=1, keepdims=True)
        uext = jnp.where(lane == i, column, uext)
    ucols[mine, :] = uext.astype(BF16)
    for load in loads[3:]:
        load.wait()
    pl.semaphore_wait(barrier, len(peers))

    def gather_weight(i, ref):
        def ref_at(dev, s):
            return ref.at[pl.ds(pl.multiple_of(dev * wr, wr), wr), pl.ds(s[0], s[1] - s[0])]

        tiles = ref.shape[1] // LANES
        cuts = [LANES * ((tiles * k) // 4) for k in range(5)]
        return Gather(Link(p, send_sems.at[i], w_recv.at[i]), ref_at, lambda k: ref.at[pl.ds(0, k * wr)], cuts)

    ga, gb, gc = (gather_weight(i, ref) for i, ref in enumerate((wa, w1, w2)))
    for g in (ga, gb, gc):
        g.step0()
    pltpu.make_async_copy(tmine, tmine, local_sems.at[7]).wait()
    spread = Spread(Link(p, send_sems.at[3], t_recv), [send_sems.at[k] for k in (3, 4, 5)], tmine, tstage, trelay, tmid, tfinal)
    spread.pair_send()
    eye_big = (lax.broadcasted_iota(jnp.int32, (TILE, TILE), 0) == lax.broadcasted_iota(jnp.int32, (TILE, TILE), 1)).astype(BF16)

    def turn(src, dst):
        for j in range(max(src.shape) // TILE):
            at = pl.ds(j * TILE, TILE)
            if src.shape[0] > TILE:
                dst[:, at] = dot(eye_big, src[at, :], NT).astype(BF16)
            else:
                dst[at, :] = dot(eye_big, src[:, at], NT).astype(BF16)

    def start_rows():
        picked = (lax.broadcasted_iota(jnp.int32, (SUB, LANES), 1) == lax.broadcasted_iota(jnp.int32, (SUB, LANES), 0)).astype(BF16)
        ustart[...] = dot(picked, ucols[...], NT)

    def power(i, w_ref, step):
        u_row = (jnp.broadcast_to(ustart[i:i + 1, :], (SUB, width)) if step == 0 else uc[i]).astype(BF16)
        pv = dot(u_row, w_ref[...], NN)
        norm = jnp.sqrt(jnp.sum(pv * pv, axis=1, keepdims=True))
        v16 = (pv / jnp.maximum(norm, NORM_FLOOR)).astype(BF16)
        sv = dot(v16, w_ref[...], NT)
        sigma = jnp.sqrt(jnp.sum(sv * sv, axis=1, keepdims=True))
        uc[i] = sv / sigma
        if step + 1 == POWER_STEPS:
            vbuf[i, :, pl.ds(0, v16.shape[1])] = v16
        return sigma[0:1, 0:1]

    def finish_power(i, w_ref, sigma):
        v16 = vbuf[i, :, pl.ds(0, w_ref.shape[1])]
        own = dot(v16, w_ref[mine, :], NT) / sigma
        (un0_ref, un1_ref, un2_ref)[i][...] = own[0:1]
        (v0_ref, v1_ref, v2_ref)[i][...] = v16[0:1]

    def forward(w_ref, xt_ref, inv, y_ref, next_ref, mask_ref):
        for j in range(width // FTILE):
            at = pl.ds(j * FTILE, FTILE)
            y = dot(w_ref[at, :], xt_ref[...], NN) * inv
            y_ref[at, :] = y
            if next_ref is not None:
                next_ref[at, :] = jnp.where(y >= 0, y, LEAK * y).astype(BF16)
                mask_ref[at, :] = jnp.where(y >= 0, 1.0, 0.0).astype(BF16)

    acts_load.wait()
    turn(x0, xt0)
    ga.step1()
    gb.step1()
    ga.step2()
    gc.step1()
    spread.pair_take()
    ga.step3()
    gb.step2()
    spread.first_send()
    ga.step4()
    gc.step2()
    gb.step3()
    spread.first_relay()
    ga.finish()
    start_rows()
    power(0, wa.at[:, pl.ds(0, k0)], 0)
    gb.step4()
    gc.step3()
    spread.second_send()
    sa = power(0, wa.at[:, pl.ds(0, k0)], 1)
    inva = 1.0 / sa
    forward(w0, xt0, inva, yt0, xt1, mt)
    gc.step4()
    gb.finish()
    power(1, w1, 0)
    spread.second_relay()
    sb = power(1, w1, 1)
    invb = 1.0 / sb
    turn(mt, mask0)
    forward(w1, xt1, invb, yt1, xt2, mt)
    gc.finish()
    power(2, w2, 0)
    sc = power(2, w2, 1)
    invc = 1.0 / sc
    forward(w2, xt2, invc, yt2, None, None)
    turn(mt, mask1)
    spread.finish()

    lane1 = lax.broadcasted_iota(jnp.int32, (1, LANES), 1)
    sig_ref[...] = jnp.where(lane1 == 0, sa, jnp.where(lane1 == 1, sb, sc))

    scale = 1.0 / total_rows
    zero_row = jnp.zeros((1, rows), F32)

    def down(value):
        return jnp.sum(value, axis=0, keepdims=True)

    loss = zero_row
    corr = zero_row
    for j in range(side):
        at = pl.ds(j * TILE, TILE)
        y = yt2[at, :]
        residual = y - tfinal[j].reshape(TILE, rows).astype(F32)
        g = residual * scale
        lowt[at, :] = g.astype(BF16)
        loss = loss + down(residual * residual)
        corr = corr + down(g * y)
    whole = Total(Link(p, send_sems.at[9], l_recv), losssent, lossgot)
    whole.first(jnp.sum(loss, axis=1, keepdims=True))

    def share(i, x_ref, d_ref, corr):
        corr = jnp.sum(corr, axis=1, keepdims=True)
        sub = lax.broadcasted_iota(jnp.int32, (SUB, width), 0)
        uu = jnp.zeros((SUB, width), F32)
        for k, part in enumerate(split3(uc[i] * corr)):
            uu = jnp.where(sub == k, part.astype(F32), uu)
        ones = (lax.broadcasted_iota(jnp.int32, (SUB, LANES), 0) < 3).astype(BF16)
        cu[...] = dot(uu.astype(BF16), ones, TN)
        for j in range(x_ref.shape[1] // TILE):
            full = dot(lowt[...], x_ref[:, pl.ds(j * TILE, TILE)], NN)
            for k in range(TILE // LANES):
                at = pl.ds(j * TILE + k * LANES, LANES)
                v = vbuf[i, :, at].astype(F32)[0:1]
                part = full[:, k * LANES:(k + 1) * LANES] - cu[...] * v
                d_ref[:, :, :, :, at] = part.astype(BF16).reshape(side, side, CORES, wr, LANES)

    def back(w_ref, inv, low_ref, out_ref, mask_ref, next_ref):
        for j in range(w_ref.shape[1] // TILE):
            at = pl.ds(j * TILE, TILE)
            dx = (dot(low_ref[...], w_ref[:, at], NN) * inv).astype(BF16)
            out_ref[:, at] = dx
            if mask_ref is not None:
                next_ref[:, at] = jnp.where(mask_ref[:, at].astype(F32) > 0.5, dx.astype(F32), LEAK * dx.astype(F32)).astype(BF16)

    def columns(dx_ref, yt_ref):
        corr = zero_row
        for j in range(width // TILE):
            at = pl.ds(j * TILE, TILE)
            y = yt_ref[at, :]
            g = dot(eye_big, dx_ref[:, at], NT) * jnp.where(y >= 0, 1.0, LEAK)
            lowt[at, :] = g.astype(BF16)
            corr = corr + down(g * y)
        return corr

    def reducer(i, blocks, mate, relay, main, relay2, main2, acc, cols):
        return Reduce(Link(p, send_sems.at[6 + i], rs_recv.at[i]), blocks, mate, relay, main, relay2, main2, acc, cols)

    rc = reducer(2, d2, m2, ra2, rb2, rc2, re2, rf2, k1)
    rb = reducer(1, d1, m1, ra1, rb1, rc1, re1, rf1, k1)
    ra = reducer(0, d0, m0, ra0, rb0, rc0, re0, rf0, k0)
    out_rows = pl.ds(pl.multiple_of(p.me * rows, rows), rows)
    turn(lowt, low)
    back(w2, invc, low, dxa, mask1, low2)
    back(w1, invb, low2, dxb, mask0, low)
    back(w0, inva, low, dx_ref.at[out_rows], None, None)

    part = rows // DX_PARTS
    gd = []
    for i in range(DX_PARTS):
        def dx_at(dev, s, i=i):
            return dx_ref.at[pl.ds(pl.multiple_of(dev * rows + (i * part + s[0]), SUB), s[1] - s[0])]

        gd.append(Gather(Link(p, send_sems.at[10 + i], dx_recv.at[i]), dx_at, lambda k: dx_ref.at[pl.ds(0, k * part)], [part * k // 4 for k in range(5)]))
    for g in gd:
        g.step0()
    turn(xt2, x2)
    share(2, x2, d2, corr)
    rc.pair_send()
    corr = columns(dxa, yt1)
    turn(xt1, x1)
    share(1, x1, d1, corr)
    rb.pair_send()
    rc.pair_add()
    rc.far_send()
    whole.step(0)
    corr = columns(dxb, yt0)
    share(0, x0, d0, corr)
    ra.pair_send()
    rb.pair_add()
    rb.far_send()
    gd[0].step1()
    ra.pair_add()
    ra.far_send()
    whole.step(1)
    rc.far_add()
    gd[1].step1()
    rb.far_add()
    ra.far_add()
    whole.step(2)
    gd[0].step2()
    rc.near_add()
    rb.near_add()
    whole.step(3)
    gd[1].step2()
    ra.near_add()
    gd[0].step3()
    rc.far2_add()
    rb.far2_add()
    ra.far2_add()
    loss_ref[...] = whole.step(4)[0:1, 0:1] * (0.5 * scale)
    gd[1].step3()
    for i, (ref, sigma) in enumerate(((w0, sa), (w1, sb), (w2, sc))):
        finish_power(i, ref, sigma)
    gd[0].step4()
    gd[1].step4()
    rc.finish(g2_ref, invc)
    rb.finish(g1_ref, invb)
    ra.finish(g0_ref, inva)
    for g in gd:
        g.finish()
    ga.drain()
    gb.drain()
    gc.drain()
    spread.drain()
    whole.drain()
    ra.link.drain(dx_ref.at[pl.ds(0, (n - 1) * wr)])
    rb.link.drain(w1.at[pl.ds(0, (n - 1) * wr)])
    rc.link.drain(w1.at[pl.ds(0, (n - 1) * wr)])
    for g in gd:
        g.drain()


def device_program(n, acts_in, w_first, w_middle, w_last, u_first, u_middle, u_last, target):
    side = math.isqrt(n // CORES)
    total_rows, k0 = acts_in.shape
    rows = total_rows // n
    wr, k1 = w_middle.shape
    width = wr * n
    tcols = target.shape[1]
    hbm = pl.BlockSpec(memory_space=pltpu.HBM)
    chips = side * side

    def reduce_bufs(k):
        q = k // 4
        return [pltpu.VMEM((2, 2, side, wr, q), BF16), pltpu.VMEM((2, 2, side, wr, 2 * q), BF16),
                pltpu.VMEM((2, 2, wr, q), BF16), pltpu.VMEM((2, 2, wr, 2 * q), BF16), pltpu.VMEM((2, wr, 2 * q), F32)]

    vmem = pl.BlockSpec(memory_space=pltpu.VMEM)
    out_shape = (
        jax.ShapeDtypeStruct((1, 1), F32), jax.ShapeDtypeStruct((total_rows, k0), BF16),
        jax.ShapeDtypeStruct((wr, k0), F32), jax.ShapeDtypeStruct((wr, k1), F32), jax.ShapeDtypeStruct((wr, k1), F32),
        jax.ShapeDtypeStruct((1, wr), F32), jax.ShapeDtypeStruct((1, wr), F32), jax.ShapeDtypeStruct((1, wr), F32),
        jax.ShapeDtypeStruct((1, k0), BF16), jax.ShapeDtypeStruct((1, k1), BF16), jax.ShapeDtypeStruct((1, k1), BF16),
        jax.ShapeDtypeStruct((1, LANES), F32))
    scratch = [
        pltpu.VMEM((width, k0 + LANES), BF16), pltpu.VMEM((width, k1), BF16), pltpu.VMEM((width, k1), BF16),
        pltpu.VMEM((rows, k0), BF16), pltpu.VMEM((rows, k1), BF16), pltpu.VMEM((rows, k1), BF16),
        pltpu.VMEM((k0, rows), BF16), pltpu.VMEM((k1, rows), BF16), pltpu.VMEM((k1, rows), BF16),
        pltpu.VMEM((width, rows), F32), pltpu.VMEM((width, rows), F32), pltpu.VMEM((width, rows), F32),
        pltpu.VMEM((width, rows), BF16), pltpu.VMEM((rows, width), BF16), pltpu.VMEM((rows, width), BF16),
        pltpu.VMEM((width, rows), BF16), pltpu.VMEM((rows, width), BF16), pltpu.VMEM((rows, width), BF16),
        pltpu.VMEM((rows, width), BF16), pltpu.VMEM((rows, width), BF16),
        pltpu.VMEM((3, SUB, width), F32), pltpu.VMEM((width, LANES), F32), pltpu.VMEM((3, SUB, k1), BF16), pltpu.VMEM((SUB, width), F32),
        pltpu.VMEM((3, 1, wr), F32),
        pltpu.VMEM((CORES, side, side, tcols, rows), BF16), pltpu.VMEM((CORES, side, side, tcols, rows), BF16),
        pltpu.VMEM((4, 2, side // 2, tcols, rows), BF16), pltpu.VMEM((2, side, side, tcols, rows), BF16),
        pltpu.VMEM((side, side, CORES, tcols, rows), BF16),
        pltpu.VMEM((5, 8, LANES), F32), pltpu.VMEM((5, 8, LANES), F32),
        pltpu.VMEM((side, side, CORES, wr, k0), BF16), pltpu.VMEM((side, side, CORES, wr, k1), BF16), pltpu.VMEM((side, side, CORES, wr, k1), BF16),
        pltpu.VMEM((side, side, wr, k0), BF16), pltpu.VMEM((side, side, wr, k1), BF16), pltpu.VMEM((side, side, wr, k1), BF16),
        *reduce_bufs(k0), *reduce_bufs(k1), *reduce_bufs(k1),
        pltpu.SemaphoreType.DMA((8,)), pltpu.SemaphoreType.DMA((10 + DX_PARTS,)),
        pltpu.SemaphoreType.DMA((3, chips)), pltpu.SemaphoreType.DMA((DX_PARTS, chips)),
        pltpu.SemaphoreType.DMA((3, 13)), pltpu.SemaphoreType.DMA((12,)), pltpu.SemaphoreType.DMA((5,)),
    ]
    small = (w_first, w_middle, w_last, u_first.reshape(1, wr), u_middle.reshape(1, wr), u_last.reshape(1, wr), target.T)
    small = [pltpu.with_memory_space_constraint(a, pltpu.HBM) for a in small]
    outs = pl.pallas_call(
        functools.partial(kernel, n),
        out_shape=out_shape,
        in_specs=[hbm] * 8,
        out_specs=(vmem,) * len(out_shape),
        scratch_shapes=scratch,
        compiler_params=pltpu.CompilerParams(collective_id=0, has_side_effects=True, vmem_limit_bytes=VMEM_LIMIT),
        name="stack",
    )(acts_in, *small)
    final = tuple(jax.ShapeDtypeStruct(shape, dtype) for shape, dtype in (
        ((1,), F32), ((total_rows, k0), BF16), ((wr, k0), F32), ((wr, k1), F32), ((wr, k1), F32),
        ((wr,), F32), ((wr,), F32), ((wr,), F32), ((k0,), BF16), ((k1,), BF16), ((k1,), BF16), ((3,), F32)))
    return pl.pallas_call(
        emit,
        out_shape=final,
        in_specs=[vmem] * len(final),
        out_specs=tuple(hbm if 1 <= i <= 4 else vmem for i in range(len(final))),
        scratch_shapes=[pltpu.SemaphoreType.DMA((3 + EMIT_PARTS,))],
        compiler_params=pltpu.CompilerParams(vmem_limit_bytes=EMIT_LIMIT),
        name="emit",
    )(*outs)


def emit(*refs):
    count = (len(refs) - 1) // 2
    ins, outs, sems = refs[:count], refs[count:2 * count], refs[-1]
    part = ins[1].shape[0] // EMIT_PARTS
    copies = [pltpu.make_async_copy(ins[1].at[pl.ds(k * part, part)], outs[1].at[pl.ds(k * part, part)], sems.at[3 + k]) for k in range(EMIT_PARTS)]
    copies += [pltpu.make_async_copy(ins[i], outs[i], sems.at[i - 2]) for i in range(2, 5)]
    for copy in copies:
        copy.start()
    for i in (0, *range(5, count)):
        outs[i][...] = ins[i][0, 0:outs[i].shape[0]]
    for copy in copies:
        copy.wait()


def solution(mesh):
    n = mesh.shape["model"]
    row_spec = P("rep", None)
    weight_spec = P(("rep", "model"), None)
    vector_spec = P(("rep", "model"))
    group_spec = P("rep")
    in_specs = (row_spec, weight_spec, weight_spec, weight_spec, vector_spec, vector_spec, vector_spec, P("rep", "model"))
    out_specs = (group_spec, row_spec, weight_spec, weight_spec, weight_spec, vector_spec, vector_spec, vector_spec, group_spec, group_spec, group_spec, group_spec)
    return jax.shard_map(lambda *args: device_program(n, *args), mesh=mesh, in_specs=in_specs, out_specs=out_specs, check_vma=False)
```

```python
import functools
import math

import jax
import jax.numpy as jnp
from jax import lax
from jax.experimental import pallas as pl
from jax.experimental.pallas import tpu as pltpu
from jax.sharding import PartitionSpec as P

LEAK = 0.2
NORM_FLOOR = 1e-12
POWER_STEPS = 2
MESH = pl.DeviceIdType.MESH
F32 = jnp.float32
BF16 = jnp.bfloat16
NN = (((1,), (0,)), ((), ()))
NT = (((1,), (1,)), ((), ()))
TN = (((0,), (0,)), ((), ()))
CORES = 2
LANES = 128
SUB = 16
TILE = 256
FTILE = 256
VMEM_LIMIT = 40 * 1024 * 1024
EMIT_LIMIT = 12 * 1024 * 1024
DX_PARTS = 2
XP, XM, YP, YM = (1, 0), (-1, 0), (0, 1), (0, -1)
HERE = (0, 0)
FAR = 2
TRAIL = 1


def dot(lhs, rhs, dims):
    return lax.dot_general(lhs, rhs, dims, preferred_element_type=F32)


class Place:
    def __init__(self, n):
        self.side = math.isqrt(n // CORES)
        me = lax.axis_index("model")
        self.me = me
        self.core = lax.rem(me, CORES)
        self.x = lax.rem(me // CORES, self.side)
        self.y = me // (CORES * self.side)

    def col(self, dx):
        return lax.rem(self.x + (dx + self.side), self.side)

    def row(self, dy):
        return lax.rem(self.y + (dy + self.side), self.side)

    def dev(self, rel):
        return self.at(self.col(rel[0]), self.row(rel[1]))

    def mate(self):
        return self.me + 1 - CORES * self.core

    def at(self, x, y):
        return (y * self.side + x) * CORES + self.core

    def norm(self, rel):
        s = self.side
        half = s // 2
        return tuple((r + half - 1) % s - (half - 1) for r in rel)


class Link:
    def __init__(self, place, send_sem, recv_sems):
        self.place, self.send_sem, self.recv_sems = place, send_sem, recv_sems

    def copy(self, i, src, dst, target, send_sem=None):
        return pltpu.make_async_remote_copy(
            src_ref=src, dst_ref=dst, send_sem=self.send_sem if send_sem is None else send_sem,
            recv_sem=self.recv_sems.at[i], device_id={"model": target}, device_id_type=MESH)

    def start(self, i, src, dst, target, send_sem=None):
        self.copy(i, src, dst, target, send_sem).start()

    def wait(self, i, dst):
        self.copy(i, dst, dst, self.place.mate()).wait_recv()

    def drain(self, sent, send_sem=None):
        self.copy(0, sent, sent, self.place.mate(), send_sem).wait_send()


class Gather:
    def __init__(self, link, ref_at, bulk, cuts):
        self.link, self.ref_at, self.bulk, self.place = link, ref_at, bulk, link.place
        a, b, c, d, e = cuts
        self.full, self.mid, self.outer = ((a, e),), ((b, d),), ((a, b), (d, e))
        self.half = {"x": ((a, c),), "y": ((c, e),)}
        self.fwd = {"x": ((b, c),), "y": ((c, d),)}
        self.bwd = {"x": ((a, b),), "y": ((d, e),)}

    def number(self, rel):
        return (rel[1] + 1) * self.place.side + rel[0] + 1

    def start(self, rel, spans, way):
        there = self.number(self.place.norm((rel[0] - way[0], rel[1] - way[1])))
        for s in spans:
            ref = self.ref_at(self.place.dev(rel), s)
            self.link.start(there, ref, ref, self.place.dev(way))

    def take(self, rel):
        self.link.wait(self.number(rel), self.ref_at(self.place.dev(rel), self.full[0]))

    def mate(self, rel):
        ref = self.ref_at(self.place.dev(rel), self.full[0])
        self.link.start(self.number(HERE), ref, ref, self.place.mate())

    def cross(self, rel, axis):
        for way in ((YP, YM) if axis == "x" else (XP, XM)):
            self.start(rel, self.half[axis], way)

    def relay(self, rel, axis, first):
        off = rel[0] if axis == "x" else rel[1]
        way = {("x", -1): XP, ("x", 1): XM, ("y", -1): YP, ("y", 1): YM}[(axis, off)]
        self.start(rel, (self.fwd if off < 0 else self.bwd)[first], way)

    def step0(self):
        for way in (XP, YP, XM, YM):
            self.start(HERE, self.full, way)
        self.mate(HERE)

    def step1(self):
        for way in (XP, YP, XM, YM):
            rel = (-way[0], -way[1])
            self.take(rel)
            self.start(rel, self.mid if way in (XP, YP) else self.outer, way)
            self.cross(rel, "x" if way[0] else "y")
            self.mate(rel)

    def step2(self):
        for rel, axis in (((2, 0), "x"), ((0, 2), "y")):
            self.take(rel)
            self.cross(rel, axis)
            self.mate(rel)
        for rel in ((-1, -1), (-1, 1), (1, -1), (1, 1)):
            self.take(rel)
            self.relay(rel, "y", "x")
            self.relay(rel, "x", "y")
            self.mate(rel)

    def step3(self):
        for d in (-1, 1):
            self.take((2, d))
            self.relay((2, d), "y", "x")
            self.mate((2, d))
            self.take((d, 2))
            self.relay((d, 2), "x", "y")
            self.mate((d, 2))

    def step4(self):
        self.take((2, 2))
        self.mate((2, 2))

    def finish(self):
        self.link.wait(self.number(HERE), self.bulk(self.place.side ** 2))

    def drain(self):
        self.link.drain(self.bulk(CORES * self.place.side ** 2 - 1))


class Reduce:
    def __init__(self, link, blocks, mate, relay, main, relay2, main2, acc, width):
        self.link, self.place = link, link.place
        self.blocks, self.mate = blocks, mate
        self.relay, self.main, self.relay2, self.main2, self.acc = relay, main, relay2, main2, acc
        q = width // 4
        self.q = q
        self.cols = {"x": ((q, 2 * q), (0, q), (0, 2 * q)), "y": ((2 * q, 3 * q), (3 * q, 4 * q), (2 * q, 4 * q))}

    def at(self, axis, pos, span):
        cols = pl.ds(span[0], span[1] - span[0])
        if axis == "x":
            return self.blocks.at[:, pos, self.place.core, :, cols]
        return self.blocks.at[pos, :, self.place.core, :, cols]

    def one(self, dx, dy, span):
        return self.blocks.at[self.place.row(dy), self.place.col(dx), self.place.core, :, pl.ds(span[0], span[1] - span[0])]

    def pair_send(self):
        p = self.place
        self.link.start(0, self.blocks.at[:, :, 1 - p.core], self.mate, p.mate())

    def pair_add(self):
        p = self.place
        self.link.wait(0, self.mate)
        for k in range(p.side):
            mine = self.blocks.at[k, :, p.core]
            mine[...] = (mine[...].astype(F32) + self.mate[k].astype(F32)).astype(BF16)

    def pos(self, axis, d):
        return self.place.col(d) if axis == "x" else self.place.row(d)

    def ways(self, axis):
        return (XP, XM) if axis == "x" else (YP, YM)

    def far_send(self):
        for h, axis in enumerate(("x", "y")):
            for s, way in enumerate(self.ways(axis)):
                self.link.start(1 + 2 * h + s, self.at(axis, self.pos(axis, 2), self.cols[axis][s]),
                                self.relay.at[h, s], self.place.dev(way))

    def far_add(self):
        for h, axis in enumerate(("x", "y")):
            for s, way in enumerate(self.ways(axis)):
                self.link.wait(1 + 2 * h + s, self.relay.at[h, s])
                step = 1 if s == 0 else -1
                ref = self.at(axis, self.pos(axis, step), self.cols[axis][s])
                ref[...] = (ref[...].astype(F32) + self.relay[h, s].astype(F32)).astype(BF16)
                self.link.start(5 + h, self.at(axis, self.pos(axis, step), self.cols[axis][2]),
                                self.main.at[h, s], self.place.dev(way))

    def near_add(self):
        p = self.place
        for h, (axis, cross) in enumerate((("x", "y"), ("y", "x"))):
            self.link.wait(5 + h, self.main.at[h])
            own = self.pos(cross, 0)
            span = self.cols[axis][2]
            self.acc[h] = (self.one(0, 0, span)[...].astype(F32) + self.main[h, 0, own].astype(F32)
                           + self.main[h, 1, own].astype(F32))
            ref = self.at(axis, self.pos(axis, 0), span)
            ref[...] = (ref[...].astype(F32) + self.main[h, 0].astype(F32) + self.main[h, 1].astype(F32)).astype(BF16)
            for s, way in enumerate(self.ways(cross)):
                d = (0, 2) if cross == "y" else (2, 0)
                self.link.start(7 + 2 * h + s, self.one(d[0], d[1], self.cols[axis][s]),
                                self.relay2.at[h, s], p.dev(way))

    def far2_add(self):
        p = self.place
        for h, (axis, cross) in enumerate((("x", "y"), ("y", "x"))):
            for s, way in enumerate(self.ways(cross)):
                self.link.wait(7 + 2 * h + s, self.relay2.at[h, s])
                ref = self.one(way[0], way[1], self.cols[axis][s])
                ref[...] = (ref[...].astype(F32) + self.relay2[h, s].astype(F32)).astype(BF16)
                self.link.start(11 + h, self.one(way[0], way[1], self.cols[axis][2]),
                                self.main2.at[h, s], p.dev(way))

    def finish(self, out_ref, inv):
        for h in range(2):
            self.link.wait(11 + h, self.main2.at[h])
            out_ref[:, pl.ds(2 * self.q * h, 2 * self.q)] = (
                self.acc[h] + self.main2[h, 0].astype(F32) + self.main2[h, 1].astype(F32)) * inv


class Spread:
    def __init__(self, link, send_sems, mine, stage, relay, mid, final):
        self.link, self.place, self.sems = link, link.place, send_sems
        self.mine, self.stage, self.relay, self.mid, self.final = mine, stage, relay, mid, final

    def pair_send(self):
        p = self.place
        self.link.start(0, self.mine.at[1 - p.core], self.stage.at[p.core], p.mate(), self.sems[0])

    def pair_take(self):
        p = self.place
        self.stage[p.core] = self.mine[p.core]
        self.link.wait(0, self.stage.at[1 - p.core])

    def src(self, h, pos, lo, hi):
        rest = pl.ds(lo, hi - lo)
        return self.stage.at[h, rest, pos] if h == 0 else self.stage.at[h, pos, rest]

    def first_send(self):
        p = self.place
        s2 = p.side // 2
        for h in range(2):
            here = p.x if h == 0 else p.y
            ways = (XP, XM) if h == 0 else (YP, YM)
            pos = p.col if h == 0 else p.row
            for s, way in enumerate(ways):
                self.link.start(1 + 2 * h + s, self.src(h, pos(2), s * s2, s * s2 + s2), self.relay.at[h, s], p.dev(way), self.sems[1])
            for s, way in enumerate(ways):
                d = 1 if s == 0 else -1
                self.link.start(5 + h, self.src(h, pos(d), 0, p.side), self.mid.at[h, here], p.dev(way), self.sems[1])
            self.mid[h, here] = self.src(h, here, 0, p.side)[...]

    def first_relay(self):
        p = self.place
        s2 = p.side // 2
        for h in range(2):
            ways = (XP, XM) if h == 0 else (YP, YM)
            pos = p.col if h == 0 else p.row
            for s, way in enumerate(ways):
                self.link.wait(1 + 2 * h + s, self.relay.at[h, s])
                self.link.start(5 + h, self.relay.at[h, s],
                                self.mid.at[h, pos(-1 if s == 0 else 1), pl.ds(s * s2, s2)], p.dev(way), self.sems[1])

    def second_send(self):
        p = self.place
        s2 = p.side // 2
        for h in range(2):
            self.link.wait(5 + h, self.mid.at[h, 0:p.side - 1])
            cross = p.row if h == 0 else p.col
            ways = (YP, YM) if h == 0 else (XP, XM)
            for s, way in enumerate(ways):
                self.link.start(7 + 2 * h + s, self.mid.at[h, pl.ds(s * s2, s2), cross(2)],
                                self.relay.at[2 + h, s], p.dev(way), self.sems[2])
            for s, way in enumerate(ways):
                self.link.start(11, self.mid.at[h, :, cross(1 if s == 0 else -1)],
                                self.dst(h, cross(0), 0, p.side), p.dev(way), self.sems[2])
            self.dst(h, cross(0), 0, p.side)[...] = self.mid[h, :, cross(0)]

    def dst(self, h, pos, lo, hi):
        rest = pl.ds(lo, hi - lo)
        return self.final.at[pos, rest, h] if h == 0 else self.final.at[rest, pos, h]

    def second_relay(self):
        p = self.place
        s2 = p.side // 2
        for h in range(2):
            cross = p.row if h == 0 else p.col
            ways = (YP, YM) if h == 0 else (XP, XM)
            for s, way in enumerate(ways):
                self.link.wait(7 + 2 * h + s, self.relay.at[2 + h, s])
                self.link.start(11, self.relay.at[2 + h, s],
                                self.dst(h, cross(-1 if s == 0 else 1), s * s2, s * s2 + s2), p.dev(way), self.sems[2])

    def finish(self):
        self.link.wait(11, self.mid.at[:, 0:self.place.side - 1])

    def drain(self):
        self.link.drain(self.mine.at[0], self.sems[0])
        self.link.drain(self.mid, self.sems[1])
        self.link.drain(self.mid, self.sems[2])


class Total:
    def __init__(self, link, sent, got):
        self.link, self.place, self.sent, self.got = link, link.place, sent, got
        p = self.place
        odd = lambda c: c + 1 - 2 * lax.rem(c, 2)
        self.targets = [p.mate(), p.at(odd(p.x), p.y), p.at(p.side - 1 - p.x, p.y), p.at(p.x, odd(p.y)), p.at(p.x, p.side - 1 - p.y)]

    def send(self, i):
        self.link.start(i, self.sent.at[i], self.got.at[i], self.targets[i])

    def first(self, value):
        self.sent[0] = jnp.broadcast_to(value, self.sent.shape[1:])
        self.send(0)

    def step(self, i):
        self.link.wait(i, self.got.at[i])
        value = self.sent[i] + self.got[i]
        if i + 1 < len(self.targets):
            self.sent[i + 1] = value
            self.send(i + 1)
        return value

    def drain(self):
        self.link.drain(self.sent)


def down(value):
    return jnp.sum(value, axis=0, keepdims=True)


def along(value):
    return jnp.sum(value, axis=1, keepdims=True)


def split3(value):
    hi = value.astype(BF16)
    rest = value - hi.astype(F32)
    mid = rest.astype(BF16)
    lo = (rest - mid.astype(F32)).astype(BF16)
    return hi, mid, lo


def kernel(n, acts_hbm, w0_hbm, w1_hbm, w2_hbm, u0_hbm, u1_hbm, u2_hbm, target_hbm,
           loss_ref, dx_ref, g0_ref, g1_ref, g2_ref, un0_ref, un1_ref, un2_ref, v0_ref, v1_ref, v2_ref, sig_ref,
           wa, wb, x0, x1, x2, xt0, xt1, xt2, yt0, yt1, yt2, mt, mask0, mask1, lowt, low, low2, dxa, dxb, uv, cu, ustart,
           ubuf, tmine, tstage, trelay, tmid, tfinal, losssent, lossgot,
           d0, d1, d2, m0, m1, m2,
           ra0, rb0, rc0, re0, rf0, ra1, rb1, rc1, re1, rf1, ra2, rb2, rc2, re2, rf2,
           local_sems, send_sems, w_recv, dx_recv, rs_recv, t_recv, l_recv, o_recv):
    p = Place(n)
    side = p.side
    rows = x0.shape[0]
    wr = w0_hbm.shape[0]
    total_rows, k0 = dx_ref.shape
    k1 = wb.shape[2]
    w1, w2 = wb.at[0], wb.at[1]
    width = wa.shape[0]
    mine = pl.ds(pl.multiple_of(p.me * wr, wr), wr)
    w0 = wa.at[:, pl.ds(0, k0)]
    ucols = wa.at[:, pl.ds(k0, LANES)]

    loads = [
        pltpu.make_async_copy(u0_hbm, ubuf.at[0], local_sems.at[0]),
        pltpu.make_async_copy(u1_hbm, ubuf.at[1], local_sems.at[1]),
        pltpu.make_async_copy(u2_hbm, ubuf.at[2], local_sems.at[2]),
        pltpu.make_async_copy(w0_hbm, w0.at[mine], local_sems.at[3]),
        pltpu.make_async_copy(w1_hbm, w1.at[mine], local_sems.at[4]),
        pltpu.make_async_copy(w2_hbm, w2.at[mine], local_sems.at[5]),
    ]
    for load in loads:
        load.start()
    acts_load = pltpu.make_async_copy(acts_hbm.at[pl.ds(pl.multiple_of(p.me * rows, rows), rows)], x0, local_sems.at[6])
    acts_load.start()
    for j in range(n):
        part = tmine.at[j % CORES, j // (CORES * side), (j // CORES) % side]
        pltpu.make_async_copy(target_hbm.at[:, pl.ds(j * rows, rows)], part, local_sems.at[7]).start()

    barrier = pltpu.get_barrier_semaphore()
    peers = [p.dev(way) for way in (XP, XM, YP, YM)] + [p.mate()]
    for peer in peers:
        pl.semaphore_signal(barrier, inc=1, device_id={"model": peer}, device_id_type=MESH)
    lane = lax.broadcasted_iota(jnp.int32, (wr, LANES), 1)
    eye = (lax.broadcasted_iota(jnp.int32, (wr, wr), 0) == lax.broadcasted_iota(jnp.int32, (wr, wr), 1))
    uext = jnp.zeros((wr, LANES), F32)
    for i in range(3):
        loads[i].wait()
        column = along(jnp.where(eye, jnp.broadcast_to(ubuf[i], (wr, wr)), 0.0))
        uext = jnp.where(lane == i, column, uext)
    ucols[mine, :] = uext.astype(BF16)
    for load in loads[3:]:
        load.wait()
    pl.semaphore_wait(barrier, len(peers))

    def gather_weight(i, ref):
        def ref_at(dev, s):
            return ref.at[pl.ds(pl.multiple_of(dev * wr, wr), wr), pl.ds(s[0], s[1] - s[0])]

        tiles = ref.shape[1] // LANES
        cuts = [LANES * ((tiles * k) // 4) for k in range(5)]
        return Gather(Link(p, send_sems.at[i], w_recv.at[i]), ref_at, lambda k: ref.at[pl.ds(0, k * wr)], cuts)

    ga, gb, gc = (gather_weight(i, ref) for i, ref in enumerate((wa, w1, w2)))
    for g in (ga, gb, gc):
        g.step0()
    pltpu.make_async_copy(tmine, tmine, local_sems.at[7]).wait()
    spread = Spread(Link(p, send_sems.at[3], t_recv), [send_sems.at[k] for k in (3, 4, 5)], tmine, tstage, trelay, tmid, tfinal)
    spread.pair_send()
    eye_big = (lax.broadcasted_iota(jnp.int32, (TILE, TILE), 0) == lax.broadcasted_iota(jnp.int32, (TILE, TILE), 1)).astype(BF16)

    def turn(src, dst):
        for j in range(max(src.shape) // TILE):
            at = pl.ds(j * TILE, TILE)
            if src.shape[0] > TILE:
                dst[:, at] = dot(eye_big, src[at, :], NT).astype(BF16)
            else:
                dst[at, :] = dot(eye_big, src[:, at], NT).astype(BF16)

    def start_rows():
        picked = (lax.broadcasted_iota(jnp.int32, (SUB, LANES), 1) == lax.broadcasted_iota(jnp.int32, (SUB, LANES), 0)).astype(BF16)
        ustart[...] = dot(picked, ucols[...], NT)

    us, vs, ss = (pl.ds(k * SUB, SUB) for k in range(3))

    def power(i, w_ref, start):
        u_row = jnp.broadcast_to(start, (SUB, width)).astype(BF16)
        for step in range(POWER_STEPS):
            pv = dot(u_row, w_ref[...], NN)
            norm = jnp.sqrt(along(pv * pv))
            v16 = (pv / jnp.maximum(norm, NORM_FLOOR)).astype(BF16)
            sv = dot(v16, w_ref[...], NT)
            sigma = jnp.sqrt(along(sv * sv))
            u16 = sv / sigma
            u_row = u16.astype(BF16)
        uv[i, us, :] = u16
        uv[i, vs, pl.ds(0, v16.shape[1])] = v16.astype(F32)
        uv[i, ss, pl.ds(0, LANES)] = jnp.broadcast_to(sigma, (SUB, LANES))

    def sigma_of(i):
        return uv[i, ss, pl.ds(0, LANES)][0:1, 0:1]

    def finish_power(i, w_ref, sigma):
        v16 = uv[i, vs, pl.ds(0, w_ref.shape[1])].astype(BF16)
        own = dot(v16, w_ref[mine, :], NT) / sigma
        (un0_ref, un1_ref, un2_ref)[i][...] = own[0:1]
        (v0_ref, v1_ref, v2_ref)[i][...] = v16[0:1]

    def forward(w_ref, xt_ref, inv, y_ref, next_ref, mask_ref):
        for j in range(width // FTILE):
            at = pl.ds(j * FTILE, FTILE)
            y = dot(w_ref[at, :], xt_ref[...], NN) * inv
            y_ref[at, :] = y
            if next_ref is not None:
                next_ref[at, :] = jnp.where(y >= 0, y, LEAK * y).astype(BF16)
                mask_ref[at, :] = jnp.where(y >= 0, 1.0, 0.0).astype(BF16)

    acts_load.wait()
    turn(x0, xt0)
    ga.step1()
    gb.step1()
    ga.step2()
    gc.step1()
    gb.step2()
    spread.pair_take()
    ga.step3()
    spread.first_send()
    gc.step2()
    gb.step3()
    ga.step4()
    gc.step3()
    gb.step4()
    spread.first_relay()
    ga.finish()
    start_rows()
    power(0, w0, ustart[0:1, :])
    gc.step4()
    sa = sigma_of(0)
    inva = 1.0 / sa
    forward(w0, xt0, inva, yt0, xt1, mt)
    turn(mt, mask0)
    spread.second_send()
    gb.finish()
    gc.finish()
    power(1 + p.core, wb.at[p.core], jnp.where(p.core == 0, ustart[1:2, :], ustart[2:3, :]))
    other = Link(p, send_sems.at[10 + DX_PARTS], o_recv)
    other.start(0, uv.at[1 + p.core], uv.at[1 + p.core], p.mate())
    spread.second_relay()
    other.wait(0, uv.at[2 - p.core])
    sb, sc = sigma_of(1), sigma_of(2)
    invb = 1.0 / sb
    forward(w1, xt1, invb, yt1, xt2, mt)
    invc = 1.0 / sc
    forward(w2, xt2, invc, yt2, None, None)
    turn(mt, mask1)
    spread.finish()

    lane1 = lax.broadcasted_iota(jnp.int32, (1, LANES), 1)
    sig_ref[...] = jnp.where(lane1 == 0, sa, jnp.where(lane1 == 1, sb, sc))

    scale = 1.0 / total_rows
    zero_row = jnp.zeros((1, rows), F32)


    loss = zero_row
    corr = zero_row
    for j in range(side):
        at = pl.ds(j * TILE, TILE)
        y = yt2[at, :]
        residual = y - tfinal[j].reshape(TILE, rows).astype(F32)
        g = residual * scale
        lowt[at, :] = g.astype(BF16)
        loss = loss + down(residual * residual)
        corr = corr + down(g * y)
    whole = Total(Link(p, send_sems.at[9], l_recv), losssent, lossgot)
    whole.first(along(loss))

    def share(i, x_ref, d_ref, corr):
        corr = along(corr)
        sub = lax.broadcasted_iota(jnp.int32, (SUB, width), 0)
        uu = jnp.zeros((SUB, width), F32)
        for k, part in enumerate(split3(uv[i, us, :] * corr)):
            uu = jnp.where(sub == k, part.astype(F32), uu)
        ones = (lax.broadcasted_iota(jnp.int32, (SUB, LANES), 0) < 3).astype(BF16)
        cu[...] = dot(uu.astype(BF16), ones, TN)
        for j in range(x_ref.shape[1] // TILE):
            full = dot(lowt[...], x_ref[:, pl.ds(j * TILE, TILE)], NN)
            for k in range(TILE // LANES):
                at = pl.ds(j * TILE + k * LANES, LANES)
                v = uv[i, vs, at][0:1]
                part = full[:, k * LANES:(k + 1) * LANES] - cu[...] * v
                d_ref[:, :, :, :, at] = part.astype(BF16).reshape(side, side, CORES, wr, LANES)

    def back(w_ref, inv, low_ref, out_ref, mask_ref, next_ref):
        for j in range(w_ref.shape[1] // TILE):
            at = pl.ds(j * TILE, TILE)
            dx = (dot(low_ref[...], w_ref[:, at], NN) * inv).astype(BF16)
            out_ref[:, at] = dx
            if mask_ref is not None:
                next_ref[:, at] = jnp.where(mask_ref[:, at].astype(F32) > 0.5, dx.astype(F32), LEAK * dx.astype(F32)).astype(BF16)

    def columns(dx_ref, yt_ref):
        corr = zero_row
        for j in range(width // TILE):
            at = pl.ds(j * TILE, TILE)
            y = yt_ref[at, :]
            g = dot(eye_big, dx_ref[:, at], NT) * jnp.where(y >= 0, 1.0, LEAK)
            lowt[at, :] = g.astype(BF16)
            corr = corr + down(g * y)
        return corr

    def reducer(i, blocks, mate, relay, main, relay2, main2, acc, cols):
        return Reduce(Link(p, send_sems.at[6 + i], rs_recv.at[i]), blocks, mate, relay, main, relay2, main2, acc, cols)

    rc = reducer(2, d2, m2, ra2, rb2, rc2, re2, rf2, k1)
    rb = reducer(1, d1, m1, ra1, rb1, rc1, re1, rf1, k1)
    ra = reducer(0, d0, m0, ra0, rb0, rc0, re0, rf0, k0)
    out_rows = pl.ds(pl.multiple_of(p.me * rows, rows), rows)
    turn(lowt, low)
    back(w2, invc, low, dxa, mask1, low2)
    back(w1, invb, low2, dxb, mask0, low)
    back(w0, inva, low, dx_ref.at[out_rows], None, None)

    part = rows // DX_PARTS
    gd = []
    for i in range(DX_PARTS):
        def dx_at(dev, s, i=i):
            return dx_ref.at[pl.ds(pl.multiple_of(dev * rows + (i * part + s[0]), SUB), s[1] - s[0])]

        gd.append(Gather(Link(p, send_sems.at[10 + i], dx_recv.at[i]), dx_at, lambda k: dx_ref.at[pl.ds(0, k * part)], [part * k // 4 for k in range(5)]))
    for g in gd:
        g.step0()
    turn(xt2, x2)
    share(2, x2, d2, corr)
    rc.pair_send()
    corr = columns(dxa, yt1)
    turn(xt1, x1)
    share(1, x1, d1, corr)
    rb.pair_send()
    rc.pair_add()
    rc.far_send()
    whole.step(0)
    corr = columns(dxb, yt0)
    share(0, x0, d0, corr)
    ra.pair_send()
    rb.pair_add()
    rb.far_send()
    gd[0].step1()
    ra.pair_add()
    ra.far_send()
    whole.step(1)
    gd[1].step1()
    rc.far_add()
    gd[0].step2()
    rb.far_add()
    ra.far_add()
    whole.step(2)
    rc.near_add()
    gd[1].step2()
    rb.near_add()
    ra.near_add()
    whole.step(3)
    gd[0].step3()
    rc.far2_add()
    gd[1].step3()
    rb.far2_add()
    ra.far2_add()
    gd[0].step4()
    gd[1].step4()
    loss_ref[...] = whole.step(4)[0:1, 0:1] * (0.5 * scale)
    for i, (ref, sigma) in enumerate(((w0, sa), (w1, sb), (w2, sc))):
        finish_power(i, ref, sigma)
    rc.finish(g2_ref, invc)
    rb.finish(g1_ref, invb)
    ra.finish(g0_ref, inva)
    for g in gd:
        g.finish()
    ga.drain()
    gb.drain()
    gc.drain()
    spread.drain()
    whole.drain()
    other.drain(uv.at[0])
    ra.link.drain(dx_ref.at[pl.ds(0, (n - 1) * wr)])
    rb.link.drain(w1.at[pl.ds(0, (n - 1) * wr)])
    rc.link.drain(w1.at[pl.ds(0, (n - 1) * wr)])
    for g in gd:
        g.drain()


def device_program(n, acts_in, w_first, w_middle, w_last, u_first, u_middle, u_last, target):
    side = math.isqrt(n // CORES)
    total_rows, k0 = acts_in.shape
    rows = total_rows // n
    wr, k1 = w_middle.shape
    width = wr * n
    tcols = target.shape[1]
    hbm = pl.BlockSpec(memory_space=pltpu.HBM)
    chips = side * side

    def reduce_bufs(k):
        q = k // 4
        return [pltpu.VMEM((2, 2, side, wr, q), BF16), pltpu.VMEM((2, 2, side, wr, 2 * q), BF16),
                pltpu.VMEM((2, 2, wr, q), BF16), pltpu.VMEM((2, 2, wr, 2 * q), BF16), pltpu.VMEM((2, wr, 2 * q), F32)]

    vmem = pl.BlockSpec(memory_space=pltpu.VMEM)
    out_shape = (
        jax.ShapeDtypeStruct((1, 1), F32), jax.ShapeDtypeStruct((total_rows, k0), BF16),
        jax.ShapeDtypeStruct((wr, k0), F32), jax.ShapeDtypeStruct((wr, k1), F32), jax.ShapeDtypeStruct((wr, k1), F32),
        jax.ShapeDtypeStruct((1, wr), F32), jax.ShapeDtypeStruct((1, wr), F32), jax.ShapeDtypeStruct((1, wr), F32),
        jax.ShapeDtypeStruct((1, k0), BF16), jax.ShapeDtypeStruct((1, k1), BF16), jax.ShapeDtypeStruct((1, k1), BF16),
        jax.ShapeDtypeStruct((1, LANES), F32))
    scratch = [
        pltpu.VMEM((width, k0 + LANES), BF16), pltpu.VMEM((2, width, k1), BF16),
        pltpu.VMEM((rows, k0), BF16), pltpu.VMEM((rows, k1), BF16), pltpu.VMEM((rows, k1), BF16),
        pltpu.VMEM((k0, rows), BF16), pltpu.VMEM((k1, rows), BF16), pltpu.VMEM((k1, rows), BF16),
        pltpu.VMEM((width, rows), F32), pltpu.VMEM((width, rows), F32), pltpu.VMEM((width, rows), F32),
        pltpu.VMEM((width, rows), BF16), pltpu.VMEM((rows, width), BF16), pltpu.VMEM((rows, width), BF16),
        pltpu.VMEM((width, rows), BF16), pltpu.VMEM((rows, width), BF16), pltpu.VMEM((rows, width), BF16),
        pltpu.VMEM((rows, width), BF16), pltpu.VMEM((rows, width), BF16),
        pltpu.VMEM((3, 3 * SUB, width), F32), pltpu.VMEM((width, LANES), F32), pltpu.VMEM((SUB, width), F32),
        pltpu.VMEM((3, 1, wr), F32),
        pltpu.VMEM((CORES, side, side, tcols, rows), BF16), pltpu.VMEM((CORES, side, side, tcols, rows), BF16),
        pltpu.VMEM((4, 2, side // 2, tcols, rows), BF16), pltpu.VMEM((2, side, side, tcols, rows), BF16),
        pltpu.VMEM((side, side, CORES, tcols, rows), BF16),
        pltpu.VMEM((5, 8, LANES), F32), pltpu.VMEM((5, 8, LANES), F32),
        pltpu.VMEM((side, side, CORES, wr, k0), BF16), pltpu.VMEM((side, side, CORES, wr, k1), BF16), pltpu.VMEM((side, side, CORES, wr, k1), BF16),
        pltpu.VMEM((side, side, wr, k0), BF16), pltpu.VMEM((side, side, wr, k1), BF16), pltpu.VMEM((side, side, wr, k1), BF16),
        *reduce_bufs(k0), *reduce_bufs(k1), *reduce_bufs(k1),
        pltpu.SemaphoreType.DMA((8,)), pltpu.SemaphoreType.DMA((11 + DX_PARTS,)),
        pltpu.SemaphoreType.DMA((3, chips)), pltpu.SemaphoreType.DMA((DX_PARTS, chips)),
        pltpu.SemaphoreType.DMA((3, 13)), pltpu.SemaphoreType.DMA((12,)), pltpu.SemaphoreType.DMA((5,)), pltpu.SemaphoreType.DMA((1,)),
    ]
    small = (w_first, w_middle, w_last, u_first.reshape(1, wr), u_middle.reshape(1, wr), u_last.reshape(1, wr), target.T)
    small = [pltpu.with_memory_space_constraint(a, pltpu.HBM) for a in small]
    outs = pl.pallas_call(
        functools.partial(kernel, n),
        out_shape=out_shape,
        in_specs=[hbm] * 8,
        out_specs=(vmem,) * len(out_shape),
        scratch_shapes=scratch,
        compiler_params=pltpu.CompilerParams(collective_id=0, has_side_effects=True, vmem_limit_bytes=VMEM_LIMIT),
        name="stack",
    )(acts_in, *small)
    final = tuple(jax.ShapeDtypeStruct(shape, dtype) for shape, dtype in (
        ((1,), F32), ((total_rows, k0), BF16), ((wr, k0), F32), ((wr, k1), F32), ((wr, k1), F32),
        ((wr,), F32), ((wr,), F32), ((wr,), F32), ((k0,), BF16), ((k1,), BF16), ((k1,), BF16), ((3,), F32)))
    return pl.pallas_call(
        functools.partial(emit, len(final)),
        out_shape=final,
        in_specs=[vmem] * len(final),
        out_specs=(hbm,) * len(final),
        scratch_shapes=[pltpu.VMEM(f.shape, f.dtype) for f in final if len(f.shape) == 1] + [pltpu.SemaphoreType.DMA((len(final),))],
        compiler_params=pltpu.CompilerParams(vmem_limit_bytes=EMIT_LIMIT),
        name="emit",
    )(*outs)


def emit(count, *refs):
    ins, outs, small, sems = refs[:count], refs[count:CORES * count], refs[CORES * count:-1], refs[-1]
    flat = [i for i in range(count) if len(outs[i].shape) < len(ins[i].shape)]
    copies = [pltpu.make_async_copy(ins[i], outs[i], sems.at[i]) for i in range(count) if i not in flat]
    for copy in copies:
        copy.start()
    for i, buf in zip(flat, small):
        buf[...] = ins[i][0, 0:outs[i].shape[0]]
        copies.append(pltpu.make_async_copy(buf, outs[i], sems.at[i]))
        copies[-1].start()
    for copy in copies:
        copy.wait()


def solution(mesh):
    n = mesh.shape["model"]
    row_spec = P("rep", None)
    weight_spec = P(("rep", "model"), None)
    vector_spec = P(("rep", "model"))
    group_spec = P("rep")
    in_specs = (row_spec, weight_spec, weight_spec, weight_spec, vector_spec, vector_spec, vector_spec, P("rep", "model"))
    out_specs = (group_spec, row_spec, weight_spec, weight_spec, weight_spec, vector_spec, vector_spec, vector_spec, group_spec, group_spec, group_spec, group_spec)
    return jax.shard_map(lambda *args: device_program(n, *args), mesh=mesh, in_specs=in_specs, out_specs=out_specs, check_vma=False)
```

```python
import functools
import math

import jax
import jax.numpy as jnp
from jax import lax
from jax.experimental import pallas as pl
from jax.experimental.pallas import tpu as pltpu
from jax.sharding import PartitionSpec as P

LEAK = 0.2
NORM_FLOOR = 1e-12
POWER_STEPS = 2
MESH = pl.DeviceIdType.MESH
F32 = jnp.float32
BF16 = jnp.bfloat16
NN = (((1,), (0,)), ((), ()))
NT = (((1,), (1,)), ((), ()))
TN = (((0,), (0,)), ((), ()))
CORES = 2
LANES = 128
SUB = 16
TILE = 256
FTILE = 256
VMEM_LIMIT = 40 * 1024 * 1024
EMIT_LIMIT = 12 * 1024 * 1024
DX_PARTS = 2
XP, XM, YP, YM = (1, 0), (-1, 0), (0, 1), (0, -1)
HERE = (0, 0)
FAR = 2
TRAIL = 1


def dot(lhs, rhs, dims):
    return lax.dot_general(lhs, rhs, dims, preferred_element_type=F32)


class Place:
    def __init__(self, n):
        self.side = math.isqrt(n // CORES)
        me = lax.axis_index("model")
        self.me = me
        self.core = lax.rem(me, CORES)
        self.x = lax.rem(me // CORES, self.side)
        self.y = me // (CORES * self.side)

    def col(self, dx):
        return lax.rem(self.x + (dx + self.side), self.side)

    def row(self, dy):
        return lax.rem(self.y + (dy + self.side), self.side)

    def dev(self, rel):
        return self.at(self.col(rel[0]), self.row(rel[1]))

    def mate(self):
        return self.me + 1 - CORES * self.core

    def at(self, x, y):
        return (y * self.side + x) * CORES + self.core

    def norm(self, rel):
        s = self.side
        half = s // 2
        return tuple((r + half - 1) % s - (half - 1) for r in rel)


class Link:
    def __init__(self, place, send_sem, recv_sems):
        self.place, self.send_sem, self.recv_sems = place, send_sem, recv_sems

    def copy(self, i, src, dst, target, send_sem=None):
        return pltpu.make_async_remote_copy(
            src_ref=src, dst_ref=dst, send_sem=self.send_sem if send_sem is None else send_sem,
            recv_sem=self.recv_sems.at[i], device_id={"model": target}, device_id_type=MESH)

    def start(self, i, src, dst, target, send_sem=None):
        self.copy(i, src, dst, target, send_sem).start()

    def wait(self, i, dst):
        self.copy(i, dst, dst, self.place.mate()).wait_recv()

    def drain(self, sent, send_sem=None):
        self.copy(0, sent, sent, self.place.mate(), send_sem).wait_send()


class Gather:
    def __init__(self, link, ref_at, bulk, cuts):
        self.link, self.ref_at, self.bulk, self.place = link, ref_at, bulk, link.place
        a, b, c, d, e = cuts
        self.full, self.mid, self.outer = ((a, e),), ((b, d),), ((a, b), (d, e))
        self.half = {"x": ((a, c),), "y": ((c, e),)}
        self.fwd = {"x": ((b, c),), "y": ((c, d),)}
        self.bwd = {"x": ((a, b),), "y": ((d, e),)}

    def number(self, rel):
        return (rel[1] + 1) * self.place.side + rel[0] + 1

    def start(self, rel, spans, way):
        there = self.number(self.place.norm((rel[0] - way[0], rel[1] - way[1])))
        for s in spans:
            ref = self.ref_at(self.place.dev(rel), s)
            self.link.start(there, ref, ref, self.place.dev(way))

    def take(self, rel):
        self.link.wait(self.number(rel), self.ref_at(self.place.dev(rel), self.full[0]))

    def mate(self, rel):
        ref = self.ref_at(self.place.dev(rel), self.full[0])
        self.link.start(self.number(HERE), ref, ref, self.place.mate())

    def cross(self, rel, axis):
        for way in ((YP, YM) if axis == "x" else (XP, XM)):
            self.start(rel, self.half[axis], way)

    def relay(self, rel, axis, first):
        off = rel[0] if axis == "x" else rel[1]
        way = {("x", -1): XP, ("x", 1): XM, ("y", -1): YP, ("y", 1): YM}[(axis, off)]
        self.start(rel, (self.fwd if off < 0 else self.bwd)[first], way)

    def step0(self):
        for way in (XP, YP, XM, YM):
            self.start(HERE, self.full, way)
        self.mate(HERE)

    def step1(self):
        for way in (XP, YP, XM, YM):
            rel = (-way[0], -way[1])
            self.take(rel)
            self.start(rel, self.mid if way in (XP, YP) else self.outer, way)
            self.cross(rel, "x" if way[0] else "y")
            self.mate(rel)

    def step2(self):
        for rel, axis in (((2, 0), "x"), ((0, 2), "y")):
            self.take(rel)
            self.cross(rel, axis)
            self.mate(rel)
        for rel in ((-1, -1), (-1, 1), (1, -1), (1, 1)):
            self.take(rel)
            self.relay(rel, "y", "x")
            self.relay(rel, "x", "y")
            self.mate(rel)

    def step3(self):
        for d in (-1, 1):
            self.take((2, d))
            self.relay((2, d), "y", "x")
            self.mate((2, d))
            self.take((d, 2))
            self.relay((d, 2), "x", "y")
            self.mate((d, 2))

    def step4(self):
        self.take((2, 2))
        self.mate((2, 2))

    def finish(self):
        self.link.wait(self.number(HERE), self.bulk(self.place.side ** 2))

    def drain(self):
        self.link.drain(self.bulk(CORES * self.place.side ** 2 - 1))


class Reduce:
    def __init__(self, link, blocks, mate, relay, main, relay2, main2, acc, width):
        self.link, self.place = link, link.place
        self.blocks, self.mate = blocks, mate
        self.relay, self.main, self.relay2, self.main2, self.acc = relay, main, relay2, main2, acc
        q = width // 4
        self.q = q
        self.cols = {"x": ((q, 2 * q), (0, q), (0, 2 * q)), "y": ((2 * q, 3 * q), (3 * q, 4 * q), (2 * q, 4 * q))}

    def at(self, axis, pos, span):
        cols = pl.ds(span[0], span[1] - span[0])
        if axis == "x":
            return self.blocks.at[:, pos, self.place.core, :, cols]
        return self.blocks.at[pos, :, self.place.core, :, cols]

    def one(self, dx, dy, span):
        return self.blocks.at[self.place.row(dy), self.place.col(dx), self.place.core, :, pl.ds(span[0], span[1] - span[0])]

    def pair_send(self):
        p = self.place
        self.link.start(0, self.blocks.at[:, :, 1 - p.core], self.mate, p.mate())

    def pair_add(self):
        p = self.place
        self.link.wait(0, self.mate)
        for k in range(p.side):
            mine = self.blocks.at[k, :, p.core]
            mine[...] = (mine[...].astype(F32) + self.mate[k].astype(F32)).astype(BF16)

    def pos(self, axis, d):
        return self.place.col(d) if axis == "x" else self.place.row(d)

    def ways(self, axis):
        return (XP, XM) if axis == "x" else (YP, YM)

    def far_send(self):
        for h, axis in enumerate(("x", "y")):
            for s, way in enumerate(self.ways(axis)):
                self.link.start(1 + 2 * h + s, self.at(axis, self.pos(axis, 2), self.cols[axis][s]),
                                self.relay.at[h, s], self.place.dev(way))

    def far_add(self):
        for h, axis in enumerate(("x", "y")):
            for s, way in enumerate(self.ways(axis)):
                self.link.wait(1 + 2 * h + s, self.relay.at[h, s])
                step = 1 if s == 0 else -1
                ref = self.at(axis, self.pos(axis, step), self.cols[axis][s])
                ref[...] = (ref[...].astype(F32) + self.relay[h, s].astype(F32)).astype(BF16)
                self.link.start(5 + h, self.at(axis, self.pos(axis, step), self.cols[axis][2]),
                                self.main.at[h, s], self.place.dev(way))

    def near_add(self):
        p = self.place
        for h, (axis, cross) in enumerate((("x", "y"), ("y", "x"))):
            self.link.wait(5 + h, self.main.at[h])
            own = self.pos(cross, 0)
            span = self.cols[axis][2]
            self.acc[h] = (self.one(0, 0, span)[...].astype(F32) + self.main[h, 0, own].astype(F32)
                           + self.main[h, 1, own].astype(F32))
            ref = self.at(axis, self.pos(axis, 0), span)
            ref[...] = (ref[...].astype(F32) + self.main[h, 0].astype(F32) + self.main[h, 1].astype(F32)).astype(BF16)
            for s, way in enumerate(self.ways(cross)):
                d = (0, 2) if cross == "y" else (2, 0)
                self.link.start(7 + 2 * h + s, self.one(d[0], d[1], self.cols[axis][s]),
                                self.relay2.at[h, s], p.dev(way))

    def far2_add(self):
        p = self.place
        for h, (axis, cross) in enumerate((("x", "y"), ("y", "x"))):
            for s, way in enumerate(self.ways(cross)):
                self.link.wait(7 + 2 * h + s, self.relay2.at[h, s])
                ref = self.one(way[0], way[1], self.cols[axis][s])
                ref[...] = (ref[...].astype(F32) + self.relay2[h, s].astype(F32)).astype(BF16)
                self.link.start(11 + h, self.one(way[0], way[1], self.cols[axis][2]),
                                self.main2.at[h, s], p.dev(way))

    def finish(self, out_ref, inv):
        for h in range(2):
            self.link.wait(11 + h, self.main2.at[h])
            out_ref[:, pl.ds(2 * self.q * h, 2 * self.q)] = (
                self.acc[h] + self.main2[h, 0].astype(F32) + self.main2[h, 1].astype(F32)) * inv


class Spread:
    def __init__(self, link, send_sems, mine, stage, relay, mid, final):
        self.link, self.place, self.sems = link, link.place, send_sems
        self.mine, self.stage, self.relay, self.mid, self.final = mine, stage, relay, mid, final

    def pair_send(self):
        p = self.place
        self.link.start(0, self.mine.at[1 - p.core], self.stage.at[p.core], p.mate(), self.sems[0])

    def pair_take(self):
        p = self.place
        self.stage[p.core] = self.mine[p.core]
        self.link.wait(0, self.stage.at[1 - p.core])

    def src(self, h, pos, lo, hi):
        rest = pl.ds(lo, hi - lo)
        return self.stage.at[h, rest, pos] if h == 0 else self.stage.at[h, pos, rest]

    def first_send(self):
        p = self.place
        s2 = p.side // 2
        for h in range(2):
            here = p.x if h == 0 else p.y
            ways = (XP, XM) if h == 0 else (YP, YM)
            pos = p.col if h == 0 else p.row
            for s, way in enumerate(ways):
                self.link.start(1 + 2 * h + s, self.src(h, pos(2), s * s2, s * s2 + s2), self.relay.at[h, s], p.dev(way), self.sems[1])
            for s, way in enumerate(ways):
                d = 1 if s == 0 else -1
                self.link.start(5 + h, self.src(h, pos(d), 0, p.side), self.mid.at[h, here], p.dev(way), self.sems[1])
            self.mid[h, here] = self.src(h, here, 0, p.side)[...]

    def first_relay(self):
        p = self.place
        s2 = p.side // 2
        for h in range(2):
            ways = (XP, XM) if h == 0 else (YP, YM)
            pos = p.col if h == 0 else p.row
            for s, way in enumerate(ways):
                self.link.wait(1 + 2 * h + s, self.relay.at[h, s])
                self.link.start(5 + h, self.relay.at[h, s],
                                self.mid.at[h, pos(-1 if s == 0 else 1), pl.ds(s * s2, s2)], p.dev(way), self.sems[1])

    def second_send(self):
        p = self.place
        s2 = p.side // 2
        for h in range(2):
            self.link.wait(5 + h, self.mid.at[h, 0:p.side - 1])
            cross = p.row if h == 0 else p.col
            ways = (YP, YM) if h == 0 else (XP, XM)
            for s, way in enumerate(ways):
                self.link.start(7 + 2 * h + s, self.mid.at[h, pl.ds(s * s2, s2), cross(2)],
                                self.relay.at[2 + h, s], p.dev(way), self.sems[2])
            for s, way in enumerate(ways):
                self.link.start(11, self.mid.at[h, :, cross(1 if s == 0 else -1)],
                                self.dst(h, cross(0), 0, p.side), p.dev(way), self.sems[2])
            self.dst(h, cross(0), 0, p.side)[...] = self.mid[h, :, cross(0)]

    def dst(self, h, pos, lo, hi):
        rest = pl.ds(lo, hi - lo)
        return self.final.at[pos, rest, h] if h == 0 else self.final.at[rest, pos, h]

    def second_relay(self):
        p = self.place
        s2 = p.side // 2
        for h in range(2):
            cross = p.row if h == 0 else p.col
            ways = (YP, YM) if h == 0 else (XP, XM)
            for s, way in enumerate(ways):
                self.link.wait(7 + 2 * h + s, self.relay.at[2 + h, s])
                self.link.start(11, self.relay.at[2 + h, s],
                                self.dst(h, cross(-1 if s == 0 else 1), s * s2, s * s2 + s2), p.dev(way), self.sems[2])

    def finish(self):
        self.link.wait(11, self.mid.at[:, 0:self.place.side - 1])

    def drain(self):
        self.link.drain(self.mine.at[0], self.sems[0])
        self.link.drain(self.mid, self.sems[1])
        self.link.drain(self.mid, self.sems[2])


class Total:
    def __init__(self, link, sent, got):
        self.link, self.place, self.sent, self.got = link, link.place, sent, got
        p = self.place
        odd = lambda c: c + 1 - 2 * lax.rem(c, 2)
        self.targets = [p.mate(), p.at(odd(p.x), p.y), p.at(p.side - 1 - p.x, p.y), p.at(p.x, odd(p.y)), p.at(p.x, p.side - 1 - p.y)]

    def send(self, i):
        self.link.start(i, self.sent.at[i], self.got.at[i], self.targets[i])

    def first(self, value):
        self.sent[0] = jnp.broadcast_to(value, self.sent.shape[1:])
        self.send(0)

    def step(self, i):
        self.link.wait(i, self.got.at[i])
        value = self.sent[i] + self.got[i]
        if i + 1 < len(self.targets):
            self.sent[i + 1] = value
            self.send(i + 1)
        return value

    def drain(self):
        self.link.drain(self.sent)


def down(value):
    return jnp.sum(value, axis=0, keepdims=True)


def along(value):
    return jnp.sum(value, axis=1, keepdims=True)


def split3(value):
    hi = value.astype(BF16)
    rest = value - hi.astype(F32)
    mid = rest.astype(BF16)
    lo = (rest - mid.astype(F32)).astype(BF16)
    return hi, mid, lo


def kernel(n, acts_hbm, w0_hbm, w1_hbm, w2_hbm, u0_hbm, u1_hbm, u2_hbm, target_hbm,
           loss_ref, dx_ref, g0_ref, g1_ref, g2_ref, un0_ref, un1_ref, un2_ref, v0_ref, v1_ref, v2_ref, sig_ref,
           wa, wb, x0, x1, x2, xt0, xt1, xt2, yt0, yt1, yt2, mt, mask0, mask1, lowt, low, low2, dxa, dxb, uv, cu, ustart,
           ubuf, tmine, tstage, trelay, tmid, tfinal, losssent, lossgot,
           d0, d1, d2, m0, m1, m2,
           ra0, rb0, rc0, re0, rf0, ra1, rb1, rc1, re1, rf1, ra2, rb2, rc2, re2, rf2,
           local_sems, send_sems, w_recv, dx_recv, rs_recv, t_recv, l_recv, o_recv):
    p = Place(n)
    side = p.side
    rows = x0.shape[0]
    wr = w0_hbm.shape[0]
    total_rows, k0 = dx_ref.shape
    k1 = wb.shape[2]
    w1, w2 = wb.at[0], wb.at[1]
    width = wa.shape[0]
    mine = pl.ds(pl.multiple_of(p.me * wr, wr), wr)
    w0 = wa.at[:, pl.ds(0, k0)]
    ucols = wa.at[:, pl.ds(k0, LANES)]

    loads = [
        pltpu.make_async_copy(u0_hbm, ubuf.at[0], local_sems.at[0]),
        pltpu.make_async_copy(u1_hbm, ubuf.at[1], local_sems.at[1]),
        pltpu.make_async_copy(u2_hbm, ubuf.at[2], local_sems.at[2]),
        pltpu.make_async_copy(w0_hbm, w0.at[mine], local_sems.at[3]),
        pltpu.make_async_copy(w1_hbm, w1.at[mine], local_sems.at[4]),
        pltpu.make_async_copy(w2_hbm, w2.at[mine], local_sems.at[5]),
    ]
    for load in loads:
        load.start()
    acts_load = pltpu.make_async_copy(acts_hbm.at[pl.ds(pl.multiple_of(p.me * rows, rows), rows)], x0, local_sems.at[6])
    acts_load.start()
    for j in range(n):
        part = tmine.at[j % CORES, j // (CORES * side), (j // CORES) % side]
        pltpu.make_async_copy(target_hbm.at[:, pl.ds(j * rows, rows)], part, local_sems.at[7]).start()

    barrier = pltpu.get_barrier_semaphore()
    peers = [p.dev(way) for way in (XP, XM, YP, YM)] + [p.mate()]
    for peer in peers:
        pl.semaphore_signal(barrier, inc=1, device_id={"model": peer}, device_id_type=MESH)
    lane = lax.broadcasted_iota(jnp.int32, (wr, LANES), 1)
    eye = (lax.broadcasted_iota(jnp.int32, (wr, wr), 0) == lax.broadcasted_iota(jnp.int32, (wr, wr), 1))
    uext = jnp.zeros((wr, LANES), F32)
    for i in range(3):
        loads[i].wait()
        column = along(jnp.where(eye, jnp.broadcast_to(ubuf[i], (wr, wr)), 0.0))
        uext = jnp.where(lane == i, column, uext)
    ucols[mine, :] = uext.astype(BF16)
    for load in loads[3:]:
        load.wait()
    pl.semaphore_wait(barrier, len(peers))

    def gather_weight(i, ref):
        def ref_at(dev, s):
            return ref.at[pl.ds(pl.multiple_of(dev * wr, wr), wr), pl.ds(s[0], s[1] - s[0])]

        tiles = ref.shape[1] // LANES
        cuts = [LANES * ((tiles * k) // 4) for k in range(5)]
        return Gather(Link(p, send_sems.at[i], w_recv.at[i]), ref_at, lambda k: ref.at[pl.ds(0, k * wr)], cuts)

    ga, gb, gc = (gather_weight(i, ref) for i, ref in enumerate((wa, w1, w2)))
    for g in (ga, gb, gc):
        g.step0()
    pltpu.make_async_copy(tmine, tmine, local_sems.at[7]).wait()
    spread = Spread(Link(p, send_sems.at[3], t_recv), [send_sems.at[k] for k in (3, 4, 5)], tmine, tstage, trelay, tmid, tfinal)
    spread.pair_send()
    eye_big = (lax.broadcasted_iota(jnp.int32, (TILE, TILE), 0) == lax.broadcasted_iota(jnp.int32, (TILE, TILE), 1)).astype(BF16)

    def turn(src, dst):
        for j in range(max(src.shape) // TILE):
            at = pl.ds(j * TILE, TILE)
            if src.shape[0] > TILE:
                dst[:, at] = dot(eye_big, src[at, :], NT).astype(BF16)
            else:
                dst[at, :] = dot(eye_big, src[:, at], NT).astype(BF16)

    def start_rows():
        picked = (lax.broadcasted_iota(jnp.int32, (SUB, LANES), 1) == lax.broadcasted_iota(jnp.int32, (SUB, LANES), 0)).astype(BF16)
        ustart[...] = dot(picked, ucols[...], NT)

    us, vs, ss = (pl.ds(k * SUB, SUB) for k in range(3))

    def power(i, w_ref, start):
        u_row = jnp.broadcast_to(start, (SUB, width)).astype(BF16)
        for step in range(POWER_STEPS):
            pv = dot(u_row, w_ref[...], NN)
            norm = jnp.sqrt(along(pv * pv))
            v16 = (pv / jnp.maximum(norm, NORM_FLOOR)).astype(BF16)
            sv = dot(v16, w_ref[...], NT)
            sigma = jnp.sqrt(along(sv * sv))
            u16 = sv / sigma
            u_row = u16.astype(BF16)
        uv[i, us, :] = u16
        uv[i, vs, pl.ds(0, v16.shape[1])] = v16.astype(F32)
        uv[i, ss, pl.ds(0, LANES)] = jnp.broadcast_to(sigma, (SUB, LANES))

    def sigma_of(i):
        return uv[i, ss, pl.ds(0, LANES)][0:1, 0:1]

    def finish_power(i, w_ref, sigma):
        v16 = uv[i, vs, pl.ds(0, w_ref.shape[1])].astype(BF16)
        own = dot(v16, w_ref[mine, :], NT) / sigma
        (un0_ref, un1_ref, un2_ref)[i][...] = own[0:1]
        (v0_ref, v1_ref, v2_ref)[i][...] = v16[0:1]

    def products(w_ref, xt_ref, y_ref):
        for j in range(width // FTILE):
            at = pl.ds(j * FTILE, FTILE)
            y_ref[at, :] = dot(w_ref[at, :], xt_ref[...], NN)

    def scaled(inv, y_ref, next_ref, mask_ref):
        for j in range(width // FTILE):
            at = pl.ds(j * FTILE, FTILE)
            y = y_ref[at, :] * inv
            y_ref[at, :] = y
            next_ref[at, :] = jnp.where(y >= 0, y, LEAK * y).astype(BF16)
            mask_ref[at, :] = jnp.where(y >= 0, 1.0, 0.0).astype(BF16)

    def forward(w_ref, xt_ref, inv, y_ref, next_ref, mask_ref):
        for j in range(width // FTILE):
            at = pl.ds(j * FTILE, FTILE)
            y = dot(w_ref[at, :], xt_ref[...], NN) * inv
            y_ref[at, :] = y
            if next_ref is not None:
                next_ref[at, :] = jnp.where(y >= 0, y, LEAK * y).astype(BF16)
                mask_ref[at, :] = jnp.where(y >= 0, 1.0, 0.0).astype(BF16)

    acts_load.wait()
    turn(x0, xt0)
    ga.step1()
    gb.step1()
    ga.step2()
    gc.step1()
    gb.step2()
    spread.pair_take()
    ga.step3()
    spread.first_send()
    gc.step2()
    gb.step3()
    ga.step4()
    gc.step3()
    spread.first_relay()
    gb.step4()
    ga.finish()
    start_rows()
    power(0, w0, ustart[0:1, :])
    gc.step4()
    spread.second_send()
    sa = sigma_of(0)
    inva = 1.0 / sa
    forward(w0, xt0, inva, yt0, xt1, mt)
    turn(mt, mask0)
    gb.finish()
    gc.finish()
    power(1 + p.core, wb.at[p.core], jnp.where(p.core == 0, ustart[1:2, :], ustart[2:3, :]))
    other = Link(p, send_sems.at[10 + DX_PARTS], o_recv)
    other.start(0, uv.at[1 + p.core], uv.at[1 + p.core], p.mate())
    spread.second_relay()
    products(w1, xt1, yt1)
    other.wait(0, uv.at[2 - p.core])
    sb, sc = sigma_of(1), sigma_of(2)
    invb = 1.0 / sb
    scaled(invb, yt1, xt2, mt)
    invc = 1.0 / sc
    forward(w2, xt2, invc, yt2, None, None)
    turn(mt, mask1)
    spread.finish()

    lane1 = lax.broadcasted_iota(jnp.int32, (1, LANES), 1)
    sig_ref[...] = jnp.where(lane1 == 0, sa, jnp.where(lane1 == 1, sb, sc))

    scale = 1.0 / total_rows
    zero_row = jnp.zeros((1, rows), F32)


    loss = zero_row
    corr = zero_row
    for j in range(side):
        at = pl.ds(j * TILE, TILE)
        y = yt2[at, :]
        residual = y - tfinal[j].reshape(TILE, rows).astype(F32)
        g = residual * scale
        lowt[at, :] = g.astype(BF16)
        loss = loss + down(residual * residual)
        corr = corr + down(g * y)
    whole = Total(Link(p, send_sems.at[9], l_recv), losssent, lossgot)
    whole.first(along(loss))

    def share(i, x_ref, d_ref, corr):
        corr = along(corr)
        sub = lax.broadcasted_iota(jnp.int32, (SUB, width), 0)
        uu = jnp.zeros((SUB, width), F32)
        for k, part in enumerate(split3(uv[i, us, :] * corr)):
            uu = jnp.where(sub == k, part.astype(F32), uu)
        ones = (lax.broadcasted_iota(jnp.int32, (SUB, LANES), 0) < 3).astype(BF16)
        cu[...] = dot(uu.astype(BF16), ones, TN)
        for j in range(x_ref.shape[1] // TILE):
            full = dot(lowt[...], x_ref[:, pl.ds(j * TILE, TILE)], NN)
            for k in range(TILE // LANES):
                at = pl.ds(j * TILE + k * LANES, LANES)
                v = uv[i, vs, at][0:1]
                part = full[:, k * LANES:(k + 1) * LANES] - cu[...] * v
                d_ref[:, :, :, :, at] = part.astype(BF16).reshape(side, side, CORES, wr, LANES)

    def back(w_ref, inv, low_ref, out_ref, mask_ref, next_ref):
        for j in range(w_ref.shape[1] // TILE):
            at = pl.ds(j * TILE, TILE)
            dx = (dot(low_ref[...], w_ref[:, at], NN) * inv).astype(BF16)
            out_ref[:, at] = dx
            if mask_ref is not None:
                next_ref[:, at] = jnp.where(mask_ref[:, at].astype(F32) > 0.5, dx.astype(F32), LEAK * dx.astype(F32)).astype(BF16)

    def columns(dx_ref, yt_ref):
        corr = zero_row
        for j in range(width // TILE):
            at = pl.ds(j * TILE, TILE)
            y = yt_ref[at, :]
            g = dot(eye_big, dx_ref[:, at], NT) * jnp.where(y >= 0, 1.0, LEAK)
            lowt[at, :] = g.astype(BF16)
            corr = corr + down(g * y)
        return corr

    def reducer(i, blocks, mate, relay, main, relay2, main2, acc, cols):
        return Reduce(Link(p, send_sems.at[6 + i], rs_recv.at[i]), blocks, mate, relay, main, relay2, main2, acc, cols)

    rc = reducer(2, d2, m2, ra2, rb2, rc2, re2, rf2, k1)
    rb = reducer(1, d1, m1, ra1, rb1, rc1, re1, rf1, k1)
    ra = reducer(0, d0, m0, ra0, rb0, rc0, re0, rf0, k0)
    out_rows = pl.ds(pl.multiple_of(p.me * rows, rows), rows)
    turn(lowt, low)
    back(w2, invc, low, dxa, mask1, low2)
    back(w1, invb, low2, dxb, mask0, low)
    back(w0, inva, low, dx_ref.at[out_rows], None, None)

    part = rows // DX_PARTS
    gd = []
    for i in range(DX_PARTS):
        def dx_at(dev, s, i=i):
            return dx_ref.at[pl.ds(pl.multiple_of(dev * rows + (i * part + s[0]), SUB), s[1] - s[0])]

        gd.append(Gather(Link(p, send_sems.at[10 + i], dx_recv.at[i]), dx_at, lambda k: dx_ref.at[pl.ds(0, k * part)], [part * k // 4 for k in range(5)]))
    for g in gd:
        g.step0()
    turn(xt2, x2)
    share(2, x2, d2, corr)
    rc.pair_send()
    corr = columns(dxa, yt1)
    turn(xt1, x1)
    share(1, x1, d1, corr)
    rb.pair_send()
    rc.pair_add()
    rc.far_send()
    whole.step(0)
    corr = columns(dxb, yt0)
    share(0, x0, d0, corr)
    ra.pair_send()
    rb.pair_add()
    rb.far_send()
    gd[0].step1()
    ra.pair_add()
    ra.far_send()
    whole.step(1)
    gd[1].step1()
    rc.far_add()
    gd[0].step2()
    rb.far_add()
    ra.far_add()
    whole.step(2)
    rc.near_add()
    gd[1].step2()
    rb.near_add()
    ra.near_add()
    whole.step(3)
    gd[0].step3()
    rc.far2_add()
    gd[1].step3()
    rb.far2_add()
    ra.far2_add()
    gd[0].step4()
    gd[1].step4()
    loss_ref[...] = whole.step(4)[0:1, 0:1] * (0.5 * scale)
    for i, (ref, sigma) in enumerate(((w0, sa), (w1, sb), (w2, sc))):
        finish_power(i, ref, sigma)
    rc.finish(g2_ref, invc)
    rb.finish(g1_ref, invb)
    ra.finish(g0_ref, inva)
    for g in gd:
        g.finish()
    ga.drain()
    gb.drain()
    gc.drain()
    spread.drain()
    whole.drain()
    other.drain(uv.at[0])
    ra.link.drain(dx_ref.at[pl.ds(0, (n - 1) * wr)])
    rb.link.drain(w1.at[pl.ds(0, (n - 1) * wr)])
    rc.link.drain(w1.at[pl.ds(0, (n - 1) * wr)])
    for g in gd:
        g.drain()


def device_program(n, acts_in, w_first, w_middle, w_last, u_first, u_middle, u_last, target):
    side = math.isqrt(n // CORES)
    total_rows, k0 = acts_in.shape
    rows = total_rows // n
    wr, k1 = w_middle.shape
    width = wr * n
    tcols = target.shape[1]
    hbm = pl.BlockSpec(memory_space=pltpu.HBM)
    chips = side * side

    def reduce_bufs(k):
        q = k // 4
        return [pltpu.VMEM((2, 2, side, wr, q), BF16), pltpu.VMEM((2, 2, side, wr, 2 * q), BF16),
                pltpu.VMEM((2, 2, wr, q), BF16), pltpu.VMEM((2, 2, wr, 2 * q), BF16), pltpu.VMEM((2, wr, 2 * q), F32)]

    vmem = pl.BlockSpec(memory_space=pltpu.VMEM)
    out_shape = (
        jax.ShapeDtypeStruct((1, 1), F32), jax.ShapeDtypeStruct((total_rows, k0), BF16),
        jax.ShapeDtypeStruct((wr, k0), F32), jax.ShapeDtypeStruct((wr, k1), F32), jax.ShapeDtypeStruct((wr, k1), F32),
        jax.ShapeDtypeStruct((1, wr), F32), jax.ShapeDtypeStruct((1, wr), F32), jax.ShapeDtypeStruct((1, wr), F32),
        jax.ShapeDtypeStruct((1, k0), BF16), jax.ShapeDtypeStruct((1, k1), BF16), jax.ShapeDtypeStruct((1, k1), BF16),
        jax.ShapeDtypeStruct((1, LANES), F32))
    scratch = [
        pltpu.VMEM((width, k0 + LANES), BF16), pltpu.VMEM((2, width, k1), BF16),
        pltpu.VMEM((rows, k0), BF16), pltpu.VMEM((rows, k1), BF16), pltpu.VMEM((rows, k1), BF16),
        pltpu.VMEM((k0, rows), BF16), pltpu.VMEM((k1, rows), BF16), pltpu.VMEM((k1, rows), BF16),
        pltpu.VMEM((width, rows), F32), pltpu.VMEM((width, rows), F32), pltpu.VMEM((width, rows), F32),
        pltpu.VMEM((width, rows), BF16), pltpu.VMEM((rows, width), BF16), pltpu.VMEM((rows, width), BF16),
        pltpu.VMEM((width, rows), BF16), pltpu.VMEM((rows, width), BF16), pltpu.VMEM((rows, width), BF16),
        pltpu.VMEM((rows, width), BF16), pltpu.VMEM((rows, width), BF16),
        pltpu.VMEM((3, 3 * SUB, width), F32), pltpu.VMEM((width, LANES), F32), pltpu.VMEM((SUB, width), F32),
        pltpu.VMEM((3, 1, wr), F32),
        pltpu.VMEM((CORES, side, side, tcols, rows), BF16), pltpu.VMEM((CORES, side, side, tcols, rows), BF16),
        pltpu.VMEM((4, 2, side // 2, tcols, rows), BF16), pltpu.VMEM((2, side, side, tcols, rows), BF16),
        pltpu.VMEM((side, side, CORES, tcols, rows), BF16),
        pltpu.VMEM((5, 8, LANES), F32), pltpu.VMEM((5, 8, LANES), F32),
        pltpu.VMEM((side, side, CORES, wr, k0), BF16), pltpu.VMEM((side, side, CORES, wr, k1), BF16), pltpu.VMEM((side, side, CORES, wr, k1), BF16),
        pltpu.VMEM((side, side, wr, k0), BF16), pltpu.VMEM((side, side, wr, k1), BF16), pltpu.VMEM((side, side, wr, k1), BF16),
        *reduce_bufs(k0), *reduce_bufs(k1), *reduce_bufs(k1),
        pltpu.SemaphoreType.DMA((8,)), pltpu.SemaphoreType.DMA((11 + DX_PARTS,)),
        pltpu.SemaphoreType.DMA((3, chips)), pltpu.SemaphoreType.DMA((DX_PARTS, chips)),
        pltpu.SemaphoreType.DMA((3, 13)), pltpu.SemaphoreType.DMA((12,)), pltpu.SemaphoreType.DMA((5,)), pltpu.SemaphoreType.DMA((1,)),
    ]
    small = (w_first, w_middle, w_last, u_first.reshape(1, wr), u_middle.reshape(1, wr), u_last.reshape(1, wr), target.T)
    small = [pltpu.with_memory_space_constraint(a, pltpu.HBM) for a in small]
    outs = pl.pallas_call(
        functools.partial(kernel, n),
        out_shape=out_shape,
        in_specs=[hbm] * 8,
        out_specs=(vmem,) * len(out_shape),
        scratch_shapes=scratch,
        compiler_params=pltpu.CompilerParams(collective_id=0, has_side_effects=True, vmem_limit_bytes=VMEM_LIMIT),
        name="stack",
    )(acts_in, *small)
    final = tuple(jax.ShapeDtypeStruct(shape, dtype) for shape, dtype in (
        ((1,), F32), ((total_rows, k0), BF16), ((wr, k0), F32), ((wr, k1), F32), ((wr, k1), F32),
        ((wr,), F32), ((wr,), F32), ((wr,), F32), ((k0,), BF16), ((k1,), BF16), ((k1,), BF16), ((3,), F32)))
    return pl.pallas_call(
        functools.partial(emit, len(final)),
        out_shape=final,
        in_specs=[vmem] * len(final),
        out_specs=(hbm,) * len(final),
        scratch_shapes=[pltpu.VMEM(f.shape, f.dtype) for f in final if len(f.shape) == 1] + [pltpu.SemaphoreType.DMA((len(final),))],
        compiler_params=pltpu.CompilerParams(vmem_limit_bytes=EMIT_LIMIT),
        name="emit",
    )(*outs)


def emit(count, *refs):
    ins, outs, small, sems = refs[:count], refs[count:CORES * count], refs[CORES * count:-1], refs[-1]
    flat = [i for i in range(count) if len(outs[i].shape) < len(ins[i].shape)]
    copies = [pltpu.make_async_copy(ins[i], outs[i], sems.at[i]) for i in range(count) if i not in flat]
    for copy in copies:
        copy.start()
    for i, buf in zip(flat, small):
        buf[...] = ins[i][0, 0:outs[i].shape[0]]
        copies.append(pltpu.make_async_copy(buf, outs[i], sems.at[i]))
        copies[-1].start()
    for copy in copies:
        copy.wait()


def solution(mesh):
    n = mesh.shape["model"]
    row_spec = P("rep", None)
    weight_spec = P(("rep", "model"), None)
    vector_spec = P(("rep", "model"))
    group_spec = P("rep")
    in_specs = (row_spec, weight_spec, weight_spec, weight_spec, vector_spec, vector_spec, vector_spec, P("rep", "model"))
    out_specs = (group_spec, row_spec, weight_spec, weight_spec, weight_spec, vector_spec, vector_spec, vector_spec, group_spec, group_spec, group_spec, group_spec)
    return jax.shard_map(lambda *args: device_program(n, *args), mesh=mesh, in_specs=in_specs, out_specs=out_specs, check_vma=False)
```
